128 devices in a mesh: grp: 2 (over core), dev: 64 (over y, x, z).
Axes of the slice: x: 4, y: 4, z: 4, core: 2. Of those that a mesh axis runs over, the one named last changes fastest.
Arguments:
- accum: float32 [16384, 24, 128], P(('grp', 'dev')), may hold values from -48 to 48
- step_count: int32 [24], replicated, may hold values from 1 to 12
- stretch_slot: int32 [16384], replicated, may hold values from 0 to 16383, as said below
- span_length: int32 [128], replicated, may hold values from 1 to 256, 16384 in all
- wet_mask: int32 [32768], P(('grp', 'dev')), may hold values 0 or 1
Outputs:
- ocean_flux: float32 [32768, 24, 128], P(('grp', 'dev'))
The draws below stay inside these ranges and needn't reach their ends.
Inputs may be any that keep to these rules, and one draw needn't show every extreme that they name: `stretch_slot`: A permutation of the slots; any 128 consecutive row blocks lie on 128 different atmosphere devices (slot // 128). `span_length`: sums to 16384; some ocean device owns exactly 256 blocks. `wet_mask`: entries of slots beyond an ocean device's span are ignored.
All inputs are finite; a program needn't handle non-finite values.
Results may differ from the reference program's by a relative error of at most 0.000071.
Values sent between devices are 32-bit elements; how exact they have to be, the bound alone decides.
A program may use at most 64 MiB of HBM per device.

```python
import math
import jax
import jax.numpy as jnp
import numpy as np

FIELDS = 24
CELLS = 128
BLOCKS_DEV = 128
DEVICE_COUNT = 128
ALL_BLOCKS = 16384
CAPACITY = 256


def draw_stretch_slot(key, part):
    devices = ALL_BLOCKS // BLOCKS_DEV
    first_key = jax.random.fold_in(key, 11)
    second_key = jax.random.fold_in(key, 12)
    dealing = jax.random.permutation(first_key, devices).astype(jnp.int32)
    rotation = jax.random.randint(second_key, (devices,), 0, BLOCKS_DEV).astype(jnp.int32)
    global_ids = jnp.arange(ALL_BLOCKS, dtype=jnp.int32)
    holder = dealing[global_ids % devices]
    local_slot = (global_ids // devices + rotation[holder]) % BLOCKS_DEV
    return (holder * BLOCKS_DEV + local_slot).astype(jnp.int32)


def set_ends(drawn, own_key, least, largest):
    extent = drawn.shape
    index_at = [jax.random.randint(jax.random.fold_in(own_key, axis), (), 0, extent[axis]) for axis in range(len(extent))]
    drawn = drawn.at[tuple(index_at)].set(least)
    longest = extent.index(max(extent))
    index_at[longest] = (index_at[longest] + 1) % extent[longest]
    return drawn.at[tuple(index_at)].set(largest)


def level_of(rng, shape, cuts, low, high):
    def one(axis_at, shards_of):
        draws = jax.random.uniform(jax.random.fold_in(jax.random.fold_in(rng, 6), axis_at), (shards_of,), jnp.float32, low / len(cuts), high / len(cuts))
        return jnp.repeat(jnp.exp(draws), shape[axis_at] // shards_of).reshape((-1,) + (1,) * (len(shape) - axis_at - 1))

    factor_of = one(*cuts[0])
    for cut in cuts[1:]:
        factor_of = factor_of * one(*cut)
    return factor_of


def profile(amount, total, limit, lean):
    weights = [(1 << 20) // math.isqrt(rank ** lean) + 1 for rank in range(2, amount + 1)]
    surplus, given = total - limit - (amount - 1), [1] * (amount - 1)
    while surplus > 0:
        free = [i for i in range(amount - 1) if given[i] < limit]
        mass, remaining = sum([weights[i] for i in free]), surplus
        for i in free:
            more = min(limit - given[i], max(1, remaining * weights[i] // mass), surplus)
            given[i] = given[i] + more
            surplus = surplus - more
    return np.array([limit] + given)


def ragged(rng, number_of, total, reach, slope):
    if number_of == 2:
        one = jax.random.randint(rng, (), max(1, total - reach), min(reach, total - 1) + 1)
        return jnp.stack([one, total - one])
    tallies = jnp.asarray(profile(number_of, total, reach, slope), jnp.int32)
    twos = (number_of - 1) // 2
    source_of, receiver = tallies[1:1 + 2 * twos:2], tallies[2:2 + 2 * twos:2]
    slack = jnp.minimum(source_of - 1, reach - receiver)
    moved = jax.random.randint(jax.random.fold_in(rng, 1), (twos,), 0, 1 << 20) % (slack + 1)
    tallies = tallies.at[1:1 + 2 * twos:2].set(source_of - moved).at[2:2 + 2 * twos:2].set(receiver + moved)
    return tallies[jax.random.permutation(jax.random.fold_in(rng, 2), number_of)]


def noise(rng, shape, scale, most, pieces=(), kind=jnp.bfloat16):
    values = jax.random.normal(rng, shape, jnp.float32) * scale
    if len(pieces) > 0:
        values = level_of(rng, shape, pieces, -0.22, 0.18) * values
    return jnp.clip(values, min=-most, max=most).astype(kind)


def setup_inputs(seed: int = 0) -> dict:
    keys = jax.random.split(jax.random.key(seed), 6)
    accum = noise(keys[0], (ALL_BLOCKS, FIELDS, CELLS), 8.0, 48.0, ((0, 128),), jnp.float32)
    step_count = set_ends(jax.random.randint(keys[1], (FIELDS,), 1, 13), jax.random.fold_in(keys[1], 1), 1, 12).astype(jnp.int32)
    stretch_slot = draw_stretch_slot(jax.random.fold_in(keys[5], 71), 0)
    span_length = ragged(keys[3], DEVICE_COUNT, ALL_BLOCKS, CAPACITY, 2).astype(jnp.int32)
    wet_mask = set_ends((jax.random.randint(keys[4], (DEVICE_COUNT * CAPACITY,), 0, 4) < 3).astype(jnp.int32), jax.random.fold_in(keys[4], 1), 0, 1)
    return dict(accum=accum, step_count=step_count, stretch_slot=stretch_slot, span_length=span_length, wet_mask=wet_mask)


def reference(accum, step_count, stretch_slot, span_length, wet_mask):
    span_end = jnp.cumsum(span_length).astype(jnp.int32)
    span_start = (span_end - span_length).astype(jnp.int32)
    global_ids = jnp.arange(ALL_BLOCKS, dtype=jnp.int32)
    owner = jnp.sum((span_end[None, :] <= global_ids[:, None]).astype(jnp.int32), axis=1).astype(jnp.int32)
    position = (owner * CAPACITY + global_ids - span_start[owner]).astype(jnp.int32)
    wet = (wet_mask[position] == 1).astype(jnp.float32)
    counts = step_count.astype(jnp.float32)
    masked = (accum[stretch_slot] / counts[None, :, None]) * wet[:, None, None]
    flat = jnp.transpose(masked, (1, 0, 2)).reshape(FIELDS, ALL_BLOCKS * CELLS)
    zero_col = jnp.zeros((FIELDS, 1), jnp.float32)
    before = jnp.concatenate([zero_col, flat[:, :-1]], axis=1)
    after_cells = jnp.concatenate([flat[:, 1:], zero_col], axis=1)
    smoothed = 0.25 * before + 0.5 * flat + 0.25 * after_cells
    smoothed = jnp.transpose(smoothed.reshape(FIELDS, ALL_BLOCKS, CELLS), (1, 0, 2)) * wet[:, None, None]
    result = jnp.zeros((DEVICE_COUNT * CAPACITY, FIELDS, CELLS), jnp.float32)
    return result.at[position].set(smoothed)
```

```python
import itertools

import jax
import jax.numpy as jnp
from jax import lax
from jax.experimental import pallas as pl
from jax.experimental.pallas import tpu as pltpu
from jax.sharding import PartitionSpec as P

MESH = pl.DeviceIdType.MESH
SIDE = 4
CHIPS = SIDE**3
DEVICES = 2 * CHIPS
GROUP = 8


DISTANCES = sorted(itertools.product(range(SIDE // 2 + 1), repeat=3), key=lambda d: -sum(d))


def partners_at(distance, me, visit):
    both_ways = [axis for axis, step in enumerate(distance) if step == 1]

    def one(number, carry):
        signs = dict.fromkeys(range(3), 1)
        for bit, axis in enumerate(both_ways):
            signs[axis] = 1 - 2 * ((number // 2 ** (bit + 1)) % 2)
        steps = [distance[axis] * signs[axis] + SIDE for axis in range(3)]
        visit(partner((number % 2, *steps), me))
        return carry

    lax.fori_loop(0 if any(distance) else 1, 2 ** (len(both_ways) + 1), one, 0)


def partner(offset, me):
    core, y, x, z = ((at + step) % size for at, step, size in zip(me, offset, (2, SIDE, SIDE, SIDE)))
    return core, (y * SIDE + x) * SIDE + z


def kernel(
    accum_hbm,
    slot_ref,
    slot_hbm,
    length_ref,
    wet_ref,
    count_ref,
    out_ref,
    accum,
    send,
    recv_0,
    recv_1,
    recv_2,
    edge_send,
    edge_recv,
    picks,
    picks_smem,
    slot_smem,
    from_smem,
    wet_smem,
    last_smem,
    accum_sem,
    picks_sem,
    slot_sem,
    send_sem,
    recv_sem,
    edge_send_sem,
    edge_recv_sem,
):
    groups = send.shape[0]
    recvs = (recv_0, recv_1, recv_2)
    blocks = accum.shape[0]
    core, chip = lax.axis_index("grp"), lax.axis_index("dev")
    me = (core, chip // (SIDE * SIDE), (chip // SIDE) % SIDE, chip % SIDE)
    mine = core * CHIPS + chip

    barrier = pltpu.get_barrier_semaphore()

    def greet(step, carry):
        other = (mine + step) % DEVICES
        pl.semaphore_signal(barrier, 1, device_id=(other // CHIPS, other % CHIPS), device_id_type=MESH)
        return carry

    lax.fori_loop(1, DEVICES, greet, 0)
    accum_copy = pltpu.make_async_copy(accum_hbm, accum, accum_sem)
    accum_copy.start()
    slot_copy = pltpu.make_async_copy(slot_hbm, slot_smem, slot_sem)
    slot_copy.start()

    row = lax.broadcasted_iota(jnp.int32, (128, 128), 0)
    lane = lax.broadcasted_iota(jnp.int32, (128, 128), 1)
    length = length_ref[...]
    length_col = jnp.sum(jnp.where(row == lane, length, 0), axis=1, keepdims=True)
    end = jnp.sum(jnp.where(row <= lane, length_col, 0), axis=0, keepdims=True)
    start = end - length
    slot = slot_ref[...]
    held = (slot >> 7) == mine
    column = jnp.sum(jnp.where(held, lane, 0), axis=1, keepdims=True)
    local = jnp.sum(jnp.where(held, slot & 127, 0), axis=1, keepdims=True)
    order = row * 128 + column - start
    inside = (order >= 0) & (order < length)
    for rank in range(2):
        chosen = inside & ((order >= 128) == (rank == 1))
        picks[rank : rank + 1, :] = jnp.sum(jnp.where(chosen, local, 0), axis=0, keepdims=True)
    picks_copy = pltpu.make_async_copy(picks, picks_smem, picks_sem)
    picks_copy.start()
    at_me = lax.broadcasted_iota(jnp.int32, (1, 128), 1) == mine
    my_start = jnp.sum(jnp.where(at_me, start, 0))
    my_length = jnp.sum(jnp.where(at_me, length, 0))
    picks_copy.wait()
    accum_copy.wait()

    def pack(owner, carry):
        for rank in range(2):
            block = accum[picks_smem[rank, owner]]
            for group in range(groups):
                send[group, owner, rank] = block[group * GROUP : (group + 1) * GROUP]
        return carry

    lax.fori_loop(0, DEVICES, pack, 0, unroll=4)
    for group in range(groups):
        recvs[group][mine] = send[group, mine]
    pl.semaphore_wait(barrier, DEVICES - 1)

    for group in range(groups):

        def post(other, group=group):
            pltpu.make_async_remote_copy(
                src_ref=send.at[group, other[0] * CHIPS + other[1]],
                dst_ref=recvs[group].at[mine],
                send_sem=send_sem,
                recv_sem=recv_sem.at[group],
                device_id=other,
                device_id_type=MESH,
            ).start()

        for distance in DISTANCES:
            partners_at(distance, me, post)

    slot_copy.wait()

    def table(index, carry):
        block = jnp.minimum(my_start + index, DEVICES * blocks - 1)
        from_smem[index] = slot_smem[block >> 7, block & 127] >> 7
        valid = (index < my_length) & (wet_ref[index >> 7, index & 127] == 1)
        wet_smem[index] = jnp.where(valid, 1.0, 0.0)
        last_smem[index] = jnp.where(index == my_length - 1, 1.0, 0.0)
        return carry

    lax.fori_loop(0, 2 * 128, table, 0, unroll=4)

    field_row = lax.broadcasted_iota(jnp.int32, (groups * GROUP, 128), 0)
    field_lane = lax.broadcasted_iota(jnp.int32, (groups * GROUP, 128), 1)
    scale = 1.0 / jnp.sum(
        jnp.where(field_row == field_lane, count_ref[...].astype(jnp.float32), 0.0), axis=1, keepdims=True
    )
    at_lane = lax.broadcasted_iota(jnp.int32, (GROUP, 128), 1)
    first_lane, last_lane = at_lane == 0, at_lane == 127
    has_left = jnp.where(mine > 0, 1.0, 0.0)
    has_right = jnp.where(mine < DEVICES - 1, 1.0, 0.0)
    after, before = (mine + 1) % DEVICES, (mine + DEVICES - 1) % DEVICES
    final = jnp.maximum(my_length, 1) - 1

    for group in range(groups):
        recv = recvs[group]
        arrived = recv.at[pl.ds(0, DEVICES - 1)]
        pltpu.make_async_copy(arrived, arrived, recv_sem.at[group]).wait()
        by_field = jnp.broadcast_to(scale[group * GROUP : (group + 1) * GROUP], (GROUP, 128))
        edge_send[group, 0] = recv[from_smem[final], final >> 7] * by_field * wet_smem[final]
        edge_send[group, 1] = recv[from_smem[0], 0] * by_field * wet_smem[0]
        copies = []
        for side, other in enumerate((after, before)):
            copy = pltpu.make_async_remote_copy(
                src_ref=edge_send.at[group, side],
                dst_ref=edge_recv.at[group, side],
                send_sem=edge_send_sem.at[group, side],
                recv_sem=edge_recv_sem.at[group, side],
                device_id=(other // CHIPS, other % CHIPS),
                device_id_type=MESH,
            )
            copy.start()
            copies.append(copy)
        for copy in copies:
            copy.wait()
        left = pltpu.roll(edge_recv[group, 0], 1, 1) * has_left
        right = pltpu.roll(edge_recv[group, 1], 127, 1) * has_right

        def value(index, rank, recv=recv, by_field=by_field):
            return recv[from_smem[index], rank] * (by_field * wet_smem[index])

        def smooth(index, next_rank, carry):
            current, to_right, to_left, previous = carry
            if next_rank is None:
                following = jnp.zeros_like(current)
            else:
                following = value(index + 1, next_rank)
            next_right, next_left = pltpu.roll(following, 1, 1), pltpu.roll(following, 127, 1)
            before_cell = jnp.where(first_lane, previous, to_right)
            after_cell = jnp.where(last_lane, next_left + last_smem[index] * right, to_left)
            smoothed = 0.5 * current + 0.25 * (before_cell + after_cell)
            out_ref[index, group * GROUP : (group + 1) * GROUP, :] = smoothed * wet_smem[index]
            return following, next_right, next_left, to_right

        current = value(0, 0)
        carry = (current, pltpu.roll(current, 1, 1), pltpu.roll(current, 127, 1), left)
        carry = lax.fori_loop(0, 127, lambda i, c: smooth(i, 0, c), carry)
        carry = lax.fori_loop(127, 255, lambda i, c: smooth(i, 1, c), carry)
        smooth(255, None, carry)

    sent = send.at[0, pl.ds(0, DEVICES - 1)]

    def drain(group, carry):
        pltpu.make_async_copy(sent, sent, send_sem).wait()
        return carry

    lax.fori_loop(0, groups, drain, 0)


def on_device(accum, step_count, stretch_slot, span_length, wet_mask):
    blocks, fields, cells = accum.shape
    capacity = wet_mask.shape[0]
    groups = fields // GROUP
    slots = stretch_slot.reshape(-1, 128)
    counts = jnp.pad(step_count, (0, 128 - fields), constant_values=1).reshape(1, 128)
    vmem, smem, anywhere = (pl.BlockSpec(memory_space=m) for m in (pltpu.VMEM, pltpu.SMEM, pl.ANY))
    return pl.pallas_call(
        kernel,
        out_shape=jax.ShapeDtypeStruct((capacity, fields, cells), jnp.float32),
        in_specs=[anywhere, vmem, anywhere, vmem, smem, vmem],
        out_specs=vmem,
        scratch_shapes=[
            pltpu.VMEM((blocks, fields, cells), jnp.float32),
            pltpu.VMEM((groups, DEVICES, 2, GROUP, cells), jnp.float32),
            *[pltpu.VMEM((DEVICES, 2, GROUP, cells), jnp.float32)] * groups,
            pltpu.VMEM((groups, 2, GROUP, cells), jnp.float32),
            pltpu.VMEM((groups, 2, GROUP, cells), jnp.float32),
            pltpu.VMEM((2, 128), jnp.int32),
            pltpu.SMEM((2, 128), jnp.int32),
            pltpu.SMEM((128, 128), jnp.int32),
            pltpu.SMEM((capacity,), jnp.int32),
            pltpu.SMEM((capacity,), jnp.float32),
            pltpu.SMEM((capacity,), jnp.float32),
            pltpu.SemaphoreType.DMA,
            pltpu.SemaphoreType.DMA,
            pltpu.SemaphoreType.DMA,
            pltpu.SemaphoreType.DMA,
            pltpu.SemaphoreType.DMA((groups,)),
            pltpu.SemaphoreType.DMA((groups, 2)),
            pltpu.SemaphoreType.DMA((groups, 2)),
        ],
        compiler_params=pltpu.CompilerParams(
            collective_id=0, has_side_effects=True, vmem_limit_bytes=32 * 1024 * 1024
        ),
        name="remap",
    )(accum, slots, slots, span_length.reshape(1, -1), wet_mask.reshape(2, -1), counts)


def solution(mesh):
    return jax.shard_map(
        on_device,
        mesh=mesh,
        in_specs=(P(("grp", "dev"), None, None), P(), P(), P(), P(("grp", "dev"))),
        out_specs=P(("grp", "dev"), None, None),
        check_vma=False,
    )
```

```python
import itertools

import jax
import jax.numpy as jnp
from jax import lax
from jax.experimental import pallas as pl
from jax.experimental.pallas import tpu as pltpu
from jax.sharding import PartitionSpec as P

MESH = pl.DeviceIdType.MESH
SIDE = 4
CHIPS = SIDE**3
DEVICES = 2 * CHIPS
GROUP = 8
EDGE_GROUP = 1

DISTANCES = sorted(itertools.product(range(SIDE // 2 + 1), repeat=3), key=lambda d: -sum(d))


def partners_at(distance, turn, me, visit):
    both_ways = [axis for axis, step in enumerate(distance) if step == 1]

    def one(number, carry):
        signs = dict.fromkeys(range(3), 1)
        for bit, axis in enumerate(both_ways):
            signs[axis] = 1 - 2 * ((number // 2**bit) % 2)
        steps = (turn, *(distance[axis] * signs[axis] + SIDE for axis in range(3)))
        core, y, x, z = ((at + step) % size for at, step, size in zip(me, steps, (2, SIDE, SIDE, SIDE)))
        visit((core, (y * SIDE + x) * SIDE + z))
        return carry

    if turn or any(distance):
        lax.fori_loop(0, 2 ** len(both_ways), one, 0)


def number_of(device):
    return device[0] * CHIPS + device[1]


def device_of(number):
    return number // CHIPS, number % CHIPS


def kernel(
    accum_hbm,
    slot_hbm,
    length_hbm,
    wet_hbm,
    count_hbm,
    out_ref,
    accum,
    slot,
    length_ref,
    send_0,
    send_1,
    send_2,
    recv_0,
    recv_1,
    recv_2,
    edge_rows,
    wet_send,
    wet_recv,
    picks,
    picks_smem,
    slot_smem,
    wet_smem,
    count_smem,
    from_smem,
    take_smem,
    keep_smem,
    load_sem,
    picks_sem,
    send_sem,
    recv_sem,
    wet_send_sem,
    wet_recv_sem,
):
    sends, recvs = (send_0, send_1, send_2), (recv_0, recv_1, recv_2)
    groups = len(sends)
    blocks, fields, cells = accum.shape
    core, chip = lax.axis_index("grp"), lax.axis_index("dev")
    me = (core, chip // (SIDE * SIDE), (chip // SIDE) % SIDE, chip % SIDE)
    mine = core * CHIPS + chip

    loads = [
        pltpu.make_async_copy(src, dst, load_sem.at[number])
        for number, (src, dst) in enumerate(
            (
                (slot_hbm, slot),
                (length_hbm, length_ref),
                (accum_hbm, accum),
                (count_hbm, count_smem),
                (wet_hbm, wet_smem),
                (slot_hbm, slot_smem),
            )
        )
    ]
    for load in loads:
        load.start()
    barrier = pltpu.get_barrier_semaphore()

    def greet(step, carry):
        other = device_of((mine + step) % DEVICES)
        pl.semaphore_signal(barrier, 1, device_id=other, device_id_type=MESH)
        return carry

    lax.fori_loop(1, DEVICES, greet, 0)

    for load in loads[:2]:
        load.wait()
    row = lax.broadcasted_iota(jnp.int32, (128, 128), 0)
    lane = lax.broadcasted_iota(jnp.int32, (128, 128), 1)
    length = length_ref[...]
    length_col = jnp.sum(jnp.where(row == lane, length, 0), axis=1, keepdims=True)
    end = jnp.sum(jnp.where(row <= lane, length_col, 0), axis=0, keepdims=True)
    start = end - length
    slots = slot[...]
    held = (slots >> 7) == mine
    column = jnp.sum(jnp.where(held, lane, 0), axis=1, keepdims=True)
    local = jnp.sum(jnp.where(held, slots & 127, 0), axis=1, keepdims=True)
    order = row * 128 + column - start
    inside = (order >= 0) & (order < length)
    ahead, behind = order == -1, order == length
    for number, chosen in enumerate((inside & (order < 128), inside & (order >= 128), ahead, behind)):
        picks[number : number + 1, :] = jnp.sum(jnp.where(chosen, local, 0), axis=0, keepdims=True)
    picks_copy = pltpu.make_async_copy(picks, picks_smem, picks_sem)
    picks_copy.start()
    has_ahead = jnp.sum(jnp.where(ahead, 1.0, 0.0), axis=0, keepdims=True)
    has_behind = jnp.sum(jnp.where(behind, 1.0, 0.0), axis=0, keepdims=True)
    at_me = lax.broadcasted_iota(jnp.int32, (1, 128), 1) == mine
    my_start = jnp.sum(jnp.where(at_me, start, 0))
    my_length = jnp.sum(jnp.where(at_me, length, 0))
    final = jnp.maximum(my_length, 1) - 1

    for load in loads[3:5]:
        load.wait()
    at_field = lax.broadcasted_iota(jnp.int32, (GROUP, cells), 0)
    scales = []
    for group in range(groups):
        count = jnp.ones((GROUP, cells), jnp.int32)
        for field in range(GROUP):
            count = jnp.where(at_field == field, count_smem[group * GROUP + field], count)
        scales.append(0.25 / count.astype(jnp.float32))

    def is_wet(index):
        return wet_smem[index >> 7, index & 127] == 1

    wet_send[0] = jnp.full((GROUP, cells), jnp.where(is_wet(final), 1.0, 0.0), jnp.float32)
    wet_send[1] = jnp.full((GROUP, cells), jnp.where(is_wet(0), 1.0, 0.0), jnp.float32)

    picks_copy.wait()
    loads[2].wait()

    def pack(group):
        fields_of = slice(group * GROUP, (group + 1) * GROUP)

        def one(owner, carry):
            for rank in range(2):
                block = accum[picks_smem[rank, owner], fields_of]
                sends[group][owner, rank * GROUP : (rank + 1) * GROUP] = block * scales[group]
            return carry

        lax.fori_loop(0, DEVICES, one, 0, unroll=16)

    def keep_mine(group):
        recvs[group][mine] = sends[group][mine]

    def post(stage):
        group, turn = divmod(stage, 2)

        def to(other):
            pltpu.make_async_remote_copy(
                src_ref=sends[group].at[number_of(other)],
                dst_ref=recvs[group].at[mine],
                send_sem=send_sem.at[stage],
                recv_sem=recv_sem.at[group],
                device_id=other,
                device_id_type=MESH,
            ).start()

        for distance in DISTANCES:
            partners_at(distance, turn, me, to)

    def sent(stage):
        group, turn = divmod(stage, 2)
        those = sends[group].at[pl.ds(0, CHIPS - 1 + turn)]
        pltpu.make_async_copy(those, those, send_sem.at[stage]).wait()

    pack(0)
    keep_mine(0)
    pl.semaphore_wait(barrier, DEVICES - 1)
    wet_copies = []
    for side, step in enumerate((1, DEVICES - 1)):
        copy = pltpu.make_async_remote_copy(
            src_ref=wet_send.at[side],
            dst_ref=wet_recv.at[side],
            send_sem=wet_send_sem.at[side],
            recv_sem=wet_recv_sem.at[side],
            device_id=device_of((mine + step) % DEVICES),
            device_id_type=MESH,
        )
        copy.start()
        wet_copies.append(copy)
    post(0)
    post(1)

    all_scales = jnp.concatenate(scales, axis=0)
    wide_lane = lax.broadcasted_iota(jnp.int32, (fields, cells), 1)

    def collect(owner, carry):
        cells_ahead, cells_behind = carry
        here = wide_lane == owner
        last = accum[picks_smem[2, owner]][:, cells - 1 : cells]
        first = accum[picks_smem[3, owner]][:, 0:1]
        return jnp.where(here, last, cells_ahead), jnp.where(here, first, cells_behind)

    nothing = jnp.zeros((fields, cells), jnp.float32)
    cells_ahead, cells_behind = lax.fori_loop(0, DEVICES, collect, (nothing, nothing), unroll=8)
    gathered = jnp.concatenate(
        [
            cells_ahead * all_scales * has_ahead,
            cells_behind * all_scales * has_behind,
            jnp.zeros((128 - 2 * fields, cells), jnp.float32),
        ],
        axis=0,
    )
    edge_rows[...] = gathered.T

    def attach(owner, carry):
        sends[EDGE_GROUP][owner, 2 * GROUP : 2 * GROUP + 1] = edge_rows[pl.ds(owner, 1)]
        return carry

    lax.fori_loop(0, DEVICES, attach, 0, unroll=16)
    for group in range(1, groups):
        pack(group)
        keep_mine(group)

    loads[5].wait()

    def table(index, carry):
        block = jnp.minimum(my_start + index, DEVICES * blocks - 1)
        behind_me = index == my_length
        from_smem[index] = jnp.where(behind_me, DEVICES, slot_smem[block >> 7, block & 127] >> 7)
        keep = jnp.where((index < my_length) & is_wet(index), 1.0, 0.0)
        keep_smem[index] = keep
        take_smem[index] = jnp.where(behind_me, 1.0, keep)
        return carry

    capacity = out_ref.shape[0]
    lax.fori_loop(0, capacity, table, 0, unroll=16)
    from_smem[capacity] = DEVICES
    take_smem[capacity] = 1.0

    at_lane = lax.broadcasted_iota(jnp.int32, (GROUP, cells), 1)
    first_lane, last_lane = at_lane == 0, at_lane == cells - 1

    def arrived(group):
        those = recvs[group].at[pl.ds(0, DEVICES - 1)]
        pltpu.make_async_copy(those, those, recv_sem.at[group]).wait()

    def edges():
        def add(sender, carry):
            return carry + recvs[EDGE_GROUP][sender, 2 * GROUP : 2 * GROUP + 1]

        total = lax.fori_loop(0, DEVICES, add, jnp.zeros((1, cells), jnp.float32), unroll=16)
        lefts = []
        for group in range(groups):
            left, right = (
                jnp.sum(jnp.where(at_lane == at_field + side * fields + group * GROUP, total, 0.0), axis=1, keepdims=True)
                for side in range(2)
            )
            lefts.append(left * wet_recv[0])
            for rank in range(2):
                recvs[group][DEVICES, rank * GROUP : (rank + 1) * GROUP] = right * wet_recv[1]
        return lefts

    def smooth(group, left):
        recv = recvs[group]
        fields_of = slice(group * GROUP, (group + 1) * GROUP)

        def value(index, rank):
            return recv[from_smem[index], rank * GROUP : (rank + 1) * GROUP] * take_smem[index]

        def both(block):
            return block, pltpu.roll(block, 1, 1), pltpu.roll(block, cells - 1, 1)

        def one(index, next_rank, carry):
            (current, to_right, to_left), previous = carry
            following = both(value(index + 1, next_rank))
            cell_before = jnp.where(first_lane, previous, to_right)
            cell_after = jnp.where(last_lane, following[2], to_left)
            out_ref[index, fields_of] = ((current + current) + (cell_before + cell_after)) * keep_smem[index]
            return following, to_right

        carry = (both(value(0, 0)), left)
        half = capacity // 2
        carry = lax.fori_loop(0, half - 1, lambda i, c: one(i, 0, c), carry, unroll=16)
        lax.fori_loop(half - 1, capacity, lambda i, c: one(i, 1, c), carry, unroll=16)

    for stage in range(2):
        sent(stage)
        post(stage + 2)
    arrived(0)
    for stage in range(2, 4):
        sent(stage)
        post(stage + 2)
    arrived(1)
    for copy in wet_copies:
        copy.wait()
    lefts = edges()
    smooth(0, lefts[0])
    smooth(1, lefts[1])
    arrived(2)
    smooth(2, lefts[2])
    sent(4)
    sent(5)


def on_device(accum, step_count, stretch_slot, span_length, wet_mask):
    blocks, fields, cells = accum.shape
    capacity = wet_mask.shape[0]
    groups = fields // GROUP
    heights = [2 * GROUP + (group == EDGE_GROUP) for group in range(groups)]
    arguments = (
        accum,
        stretch_slot.reshape(-1, 128),
        span_length.reshape(1, -1),
        wet_mask.reshape(-1, 128),
        step_count,
    )
    return pl.pallas_call(
        kernel,
        out_shape=pltpu.VMEM((capacity, fields, cells), jnp.float32),
        in_specs=[pl.BlockSpec(memory_space=pltpu.HBM)] * len(arguments),
        out_specs=pl.BlockSpec(memory_space=pltpu.VMEM),
        scratch_shapes=[
            pltpu.VMEM((blocks, fields, cells), jnp.float32),
            pltpu.VMEM((128, 128), jnp.int32),
            pltpu.VMEM((1, 128), jnp.int32),
            *[pltpu.VMEM((DEVICES, height, cells), jnp.float32) for height in heights],
            *[pltpu.VMEM((DEVICES + 1, height, cells), jnp.float32) for height in heights],
            pltpu.VMEM((128, cells), jnp.float32),
            pltpu.VMEM((2, GROUP, cells), jnp.float32),
            pltpu.VMEM((2, GROUP, cells), jnp.float32),
            pltpu.VMEM((4, 128), jnp.int32),
            pltpu.SMEM((4, 128), jnp.int32),
            pltpu.SMEM((128, 128), jnp.int32),
            pltpu.SMEM((capacity // 128, 128), jnp.int32),
            pltpu.SMEM((fields,), jnp.int32),
            pltpu.SMEM((capacity + 1,), jnp.int32),
            pltpu.SMEM((capacity + 1,), jnp.float32),
            pltpu.SMEM((capacity,), jnp.float32),
            pltpu.SemaphoreType.DMA((6,)),
            pltpu.SemaphoreType.DMA,
            pltpu.SemaphoreType.DMA((2 * groups,)),
            pltpu.SemaphoreType.DMA((groups,)),
            pltpu.SemaphoreType.DMA((2,)),
            pltpu.SemaphoreType.DMA((2,)),
        ],
        compiler_params=pltpu.CompilerParams(
            collective_id=0, has_side_effects=True, vmem_limit_bytes=32 * 1024 * 1024
        ),
        name="remap",
    )(*(pltpu.with_memory_space_constraint(a, pltpu.HBM) for a in arguments))


def solution(mesh):
    return jax.shard_map(
        on_device,
        mesh=mesh,
        in_specs=(P(("grp", "dev"), None, None), P(), P(), P(), P(("grp", "dev"))),
        out_specs=P(("grp", "dev"), None, None),
        check_vma=False,
    )
```

```python
import itertools

import jax
import jax.numpy as jnp
from jax import lax
from jax.experimental import pallas as pl
from jax.experimental.pallas import tpu as pltpu
from jax.sharding import PartitionSpec as P

MESH = pl.DeviceIdType.MESH
SIDE = 4
CHIPS = SIDE**3
DEVICES = 2 * CHIPS
GROUP = 8
EDGE_GROUP = 1

DISTANCES = sorted(itertools.product(range(SIDE // 2 + 1), repeat=3), key=lambda d: -sum(d))


def partners_at(distance, turn, me, visit):
    both_ways = [axis for axis, step in enumerate(distance) if step == 1]

    def one(number, carry):
        signs = dict.fromkeys(range(3), 1)
        for bit, axis in enumerate(both_ways):
            signs[axis] = 1 - 2 * ((number // 2**bit) % 2)
        steps = (turn, *(distance[axis] * signs[axis] + SIDE for axis in range(3)))
        core, y, x, z = ((at + step) % size for at, step, size in zip(me, steps, (2, SIDE, SIDE, SIDE)))
        visit((core, (y * SIDE + x) * SIDE + z))
        return carry

    if turn or any(distance):
        lax.fori_loop(0, 2 ** len(both_ways), one, 0)


def number_of(device):
    return device[0] * CHIPS + device[1]


def device_of(number):
    return number // CHIPS, number % CHIPS


def kernel(
    accum_hbm,
    slot_hbm,
    length_hbm,
    wet_hbm,
    count_hbm,
    out_ref,
    accum,
    slot,
    length_ref,
    send_0,
    send_1,
    send_2,
    recv_0,
    recv_1,
    recv_2,
    edge_rows,
    wet_send,
    wet_recv,
    picks,
    picks_smem,
    slot_smem,
    wet_smem,
    count_smem,
    from_smem,
    take_smem,
    keep_smem,
    load_sem,
    picks_sem,
    send_sem,
    recv_sem,
    wet_send_sem,
    wet_recv_sem,
):
    sends, recvs = (send_0, send_1, send_2), (recv_0, recv_1, recv_2)
    groups = len(sends)
    blocks, fields, cells = accum.shape
    core, chip = lax.axis_index("grp"), lax.axis_index("dev")
    me = (core, chip // (SIDE * SIDE), (chip // SIDE) % SIDE, chip % SIDE)
    mine = core * CHIPS + chip

    loads = [
        pltpu.make_async_copy(src, dst, load_sem.at[number])
        for number, (src, dst) in enumerate(
            (
                (slot_hbm, slot),
                (length_hbm, length_ref),
                (accum_hbm, accum),
                (count_hbm, count_smem),
                (wet_hbm, wet_smem),
                (slot_hbm, slot_smem),
            )
        )
    ]
    for load in loads:
        load.start()
    barrier = pltpu.get_barrier_semaphore()

    def greet(step, carry):
        other = device_of((mine + step) % DEVICES)
        pl.semaphore_signal(barrier, 1, device_id=other, device_id_type=MESH)
        return carry

    lax.fori_loop(1, DEVICES, greet, 0)

    for load in loads[:2]:
        load.wait()
    row = lax.broadcasted_iota(jnp.int32, (128, 128), 0)
    lane = lax.broadcasted_iota(jnp.int32, (128, 128), 1)
    length = length_ref[...]
    length_col = jnp.sum(jnp.where(row == lane, length, 0), axis=1, keepdims=True)
    end = jnp.sum(jnp.where(row <= lane, length_col, 0), axis=0, keepdims=True)
    start = end - length
    slots = slot[...]
    held = (slots >> 7) == mine
    column = jnp.sum(jnp.where(held, lane, 0), axis=1, keepdims=True)
    local = jnp.sum(jnp.where(held, slots & 127, 0), axis=1, keepdims=True)
    order = row * 128 + column - start
    inside = (order >= 0) & (order < length)
    ahead, behind = order == -1, order == length
    for number, chosen in enumerate((inside & (order < 128), inside & (order >= 128), ahead, behind)):
        picks[number : number + 1, :] = jnp.sum(jnp.where(chosen, local, 0), axis=0, keepdims=True)
    picks_copy = pltpu.make_async_copy(picks, picks_smem, picks_sem)
    picks_copy.start()
    has_ahead = jnp.sum(jnp.where(ahead, 1.0, 0.0), axis=0, keepdims=True)
    has_behind = jnp.sum(jnp.where(behind, 1.0, 0.0), axis=0, keepdims=True)
    at_me = lax.broadcasted_iota(jnp.int32, (1, 128), 1) == mine
    my_start = jnp.sum(jnp.where(at_me, start, 0))
    my_length = jnp.sum(jnp.where(at_me, length, 0))
    final = jnp.maximum(my_length, 1) - 1

    for load in loads[3:5]:
        load.wait()
    at_field = lax.broadcasted_iota(jnp.int32, (GROUP, cells), 0)
    scales = []
    for group in range(groups):
        count = jnp.ones((GROUP, cells), jnp.int32)
        for field in range(GROUP):
            count = jnp.where(at_field == field, count_smem[group * GROUP + field], count)
        scales.append(0.25 / count.astype(jnp.float32))

    def is_wet(index):
        return wet_smem[index >> 7, index & 127] == 1

    wet_send[0] = jnp.full((GROUP, cells), jnp.where(is_wet(final), 1.0, 0.0), jnp.float32)
    wet_send[1] = jnp.full((GROUP, cells), jnp.where(is_wet(0), 1.0, 0.0), jnp.float32)

    picks_copy.wait()
    loads[2].wait()

    def pack(group):
        fields_of = slice(group * GROUP, (group + 1) * GROUP)

        def one(owner, carry):
            for rank in range(2):
                block = accum[picks_smem[rank, owner], fields_of]
                sends[group][owner, rank * GROUP : (rank + 1) * GROUP] = block * scales[group]
            return carry

        lax.fori_loop(0, DEVICES, one, 0, unroll=16)

    def keep_mine(group):
        recvs[group][mine] = sends[group][mine]

    def post(stage):
        group, turn = divmod(stage, 2)

        def to(other):
            pltpu.make_async_remote_copy(
                src_ref=sends[group].at[number_of(other)],
                dst_ref=recvs[group].at[mine],
                send_sem=send_sem.at[stage],
                recv_sem=recv_sem.at[group],
                device_id=other,
                device_id_type=MESH,
            ).start()

        for distance in DISTANCES:
            partners_at(distance, turn, me, to)

    def sent(stage):
        group, turn = divmod(stage, 2)
        those = sends[group].at[pl.ds(0, CHIPS - 1 + turn)]
        pltpu.make_async_copy(those, those, send_sem.at[stage]).wait()

    pack(0)
    keep_mine(0)
    pl.semaphore_wait(barrier, DEVICES - 1)
    wet_copies = []
    for side, step in enumerate((1, DEVICES - 1)):
        copy = pltpu.make_async_remote_copy(
            src_ref=wet_send.at[side],
            dst_ref=wet_recv.at[side],
            send_sem=wet_send_sem.at[side],
            recv_sem=wet_recv_sem.at[side],
            device_id=device_of((mine + step) % DEVICES),
            device_id_type=MESH,
        )
        copy.start()
        wet_copies.append(copy)
    post(0)
    post(1)

    all_scales = jnp.concatenate(scales, axis=0)
    wide_lane = lax.broadcasted_iota(jnp.int32, (fields, cells), 1)

    def collect(owner, carry):
        cells_ahead, cells_behind = carry
        here = wide_lane == owner
        last = accum[picks_smem[2, owner]][:, cells - 1 : cells]
        first = accum[picks_smem[3, owner]][:, 0:1]
        return jnp.where(here, last, cells_ahead), jnp.where(here, first, cells_behind)

    nothing = jnp.zeros((fields, cells), jnp.float32)
    cells_ahead, cells_behind = lax.fori_loop(0, DEVICES, collect, (nothing, nothing), unroll=8)
    gathered = jnp.concatenate(
        [
            cells_ahead * all_scales * has_ahead,
            cells_behind * all_scales * has_behind,
            jnp.zeros((128 - 2 * fields, cells), jnp.float32),
        ],
        axis=0,
    )
    edge_rows[...] = gathered.T

    def attach(owner, carry):
        sends[EDGE_GROUP][owner, 2 * GROUP : 2 * GROUP + 1] = edge_rows[pl.ds(owner, 1)]
        return carry

    lax.fori_loop(0, DEVICES, attach, 0, unroll=16)
    for group in range(1, groups):
        pack(group)
        keep_mine(group)

    loads[5].wait()

    def table(index, carry):
        block = jnp.minimum(my_start + index, DEVICES * blocks - 1)
        behind_me = index == my_length
        from_smem[index] = jnp.where(behind_me, DEVICES, slot_smem[block >> 7, block & 127] >> 7)
        keep = jnp.where((index < my_length) & is_wet(index), 1.0, 0.0)
        keep_smem[index] = keep
        take_smem[index] = jnp.where(behind_me, 1.0, keep)
        return carry

    capacity = out_ref.shape[0]
    lax.fori_loop(0, capacity, table, 0, unroll=16)
    from_smem[capacity] = DEVICES
    take_smem[capacity] = 1.0

    at_lane = lax.broadcasted_iota(jnp.int32, (GROUP, cells), 1)
    first_lane, last_lane = at_lane == 0, at_lane == cells - 1

    def arrived(group):
        those = recvs[group].at[pl.ds(0, DEVICES - 1)]
        pltpu.make_async_copy(those, those, recv_sem.at[group]).wait()

    def edges():
        def add(sender, carry):
            return carry + recvs[EDGE_GROUP][sender, 2 * GROUP : 2 * GROUP + 1]

        total = lax.fori_loop(0, DEVICES, add, jnp.zeros((1, cells), jnp.float32), unroll=16)
        lefts = []
        for group in range(groups):
            left, right = (
                jnp.sum(jnp.where(at_lane == at_field + side * fields + group * GROUP, total, 0.0), axis=1, keepdims=True)
                for side in range(2)
            )
            lefts.append(left * wet_recv[0])
            for rank in range(2):
                recvs[group][DEVICES, rank * GROUP : (rank + 1) * GROUP] = right * wet_recv[1]
        return lefts

    def smooth(group, left):
        recv = recvs[group]
        fields_of = slice(group * GROUP, (group + 1) * GROUP)

        def value(index, rank):
            return recv[from_smem[index], rank * GROUP : (rank + 1) * GROUP] * take_smem[index]

        def both(block):
            return block, pltpu.roll(block, 1, 1), pltpu.roll(block, cells - 1, 1)

        def one(index, next_rank, carry):
            (current, to_right, to_left), previous = carry
            following = both(value(index + 1, next_rank))
            cell_before = jnp.where(first_lane, previous, to_right)
            cell_after = jnp.where(last_lane, following[2], to_left)
            out_ref[index, fields_of] = ((current + current) + (cell_before + cell_after)) * keep_smem[index]
            return following, to_right

        carry = (both(value(0, 0)), left)
        half = capacity // 2
        for index in range(capacity):
            carry = one(index, 0 if index < half - 1 else 1, carry)

    for stage in range(2):
        sent(stage)
        post(stage + 2)
    arrived(0)
    for stage in range(2, 4):
        sent(stage)
        post(stage + 2)
    arrived(1)
    for copy in wet_copies:
        copy.wait()
    lefts = edges()
    smooth(0, lefts[0])
    smooth(1, lefts[1])
    arrived(2)
    smooth(2, lefts[2])
    sent(4)
    sent(5)


def on_device(accum, step_count, stretch_slot, span_length, wet_mask):
    blocks, fields, cells = accum.shape
    capacity = wet_mask.shape[0]
    groups = fields // GROUP
    heights = [2 * GROUP + (group == EDGE_GROUP) for group in range(groups)]
    arguments = (
        accum,
        stretch_slot.reshape(-1, 128),
        span_length.reshape(1, -1),
        wet_mask.reshape(-1, 128),
        step_count,
    )
    return pl.pallas_call(
        kernel,
        out_shape=pltpu.VMEM((capacity, fields, cells), jnp.float32),
        in_specs=[pl.BlockSpec(memory_space=pltpu.HBM)] * len(arguments),
        out_specs=pl.BlockSpec(memory_space=pltpu.VMEM),
        scratch_shapes=[
            pltpu.VMEM((blocks, fields, cells), jnp.float32),
            pltpu.VMEM((128, 128), jnp.int32),
            pltpu.VMEM((1, 128), jnp.int32),
            *[pltpu.VMEM((DEVICES, height, cells), jnp.float32) for height in heights],
            *[pltpu.VMEM((DEVICES + 1, height, cells), jnp.float32) for height in heights],
            pltpu.VMEM((128, cells), jnp.float32),
            pltpu.VMEM((2, GROUP, cells), jnp.float32),
            pltpu.VMEM((2, GROUP, cells), jnp.float32),
            pltpu.VMEM((4, 128), jnp.int32),
            pltpu.SMEM((4, 128), jnp.int32),
            pltpu.SMEM((128, 128), jnp.int32),
            pltpu.SMEM((capacity // 128, 128), jnp.int32),
            pltpu.SMEM((fields,), jnp.int32),
            pltpu.SMEM((capacity + 1,), jnp.int32),
            pltpu.SMEM((capacity + 1,), jnp.float32),
            pltpu.SMEM((capacity,), jnp.float32),
            pltpu.SemaphoreType.DMA((6,)),
            pltpu.SemaphoreType.DMA,
            pltpu.SemaphoreType.DMA((2 * groups,)),
            pltpu.SemaphoreType.DMA((groups,)),
            pltpu.SemaphoreType.DMA((2,)),
            pltpu.SemaphoreType.DMA((2,)),
        ],
        compiler_params=pltpu.CompilerParams(
            collective_id=0, has_side_effects=True, vmem_limit_bytes=32 * 1024 * 1024
        ),
        name="remap",
    )(*(pltpu.with_memory_space_constraint(a, pltpu.HBM) for a in arguments))


def solution(mesh):
    return jax.shard_map(
        on_device,
        mesh=mesh,
        in_specs=(P(("grp", "dev"), None, None), P(), P(), P(), P(("grp", "dev"))),
        out_specs=P(("grp", "dev"), None, None),
        check_vma=False,
    )
```

```python
import itertools

import jax
import jax.numpy as jnp
from jax import lax
from jax.experimental import pallas as pl
from jax.experimental.pallas import tpu as pltpu
from jax.sharding import PartitionSpec as P

MESH = pl.DeviceIdType.MESH
SIDE = 4
CHIPS = SIDE**3
DEVICES = 2 * CHIPS
GROUP = 8
EDGE_GROUP = 1

STEPS = sorted(
    itertools.product(range(SIDE), repeat=3),
    key=lambda steps: (2 not in steps, -sum(min(step, SIDE - step) for step in steps)),
)
FAR = sum(2 in steps for steps in STEPS)
PACKED = [
    sum((STEPS[at + k][0] * 16 + STEPS[at + k][1] * 4 + STEPS[at + k][2]) << (6 * k) for k in range(4))
    for at in range(0, CHIPS, 4)
]
STAGES = [(0, (FAR, CHIPS), (0, 1)), (0, (0, FAR), (0, 1))] + [
    (group, (0, CHIPS), (turn,)) for group in (1, 2) for turn in range(2)
]


def how_many(stage):
    _, (low, high), turns = stage
    return sum(high - low - (turn == 0 and high == CHIPS) for turn in turns)


def visit_all(stage, me, visit):
    _, (low, high), turns = stage
    core, y, x, z = me

    def one(index, carry):
        number = PACKED[0]
        for k, packed in enumerate(PACKED[1:], 1):
            number = jnp.where(index >> 2 == k, packed, number)
        number = number >> (6 * (index & 3))
        chip = (((y + (number >> 4)) & 3) * SIDE + ((x + (number >> 2)) & 3)) * SIDE + ((z + number) & 3)
        for turn in turns:
            visit(((core + turn) & 1, chip))
        return carry

    if len(turns) == 1:
        lax.fori_loop(low, min(high, CHIPS - (turns[0] == 0)), one, 0)
        return
    lax.fori_loop(low, min(high, CHIPS - 1), one, 0)
    if high == CHIPS:
        visit(((core + 1) & 1, (y * SIDE + x) * SIDE + z))


def number_of(device):
    return device[0] * CHIPS + device[1]


def device_of(number):
    return number // CHIPS, number % CHIPS


def kernel(
    accum_hbm,
    slot_hbm,
    length_hbm,
    wet_hbm,
    count_hbm,
    out_ref,
    accum,
    slot,
    length_ref,
    send_0,
    send_1,
    send_2,
    recv_0,
    recv_1,
    recv_2,
    edge_rows,
    wet_send,
    wet_recv,
    picks,
    picks_smem,
    slot_smem,
    wet_smem,
    count_smem,
    from_smem,
    take_smem,
    keep_smem,
    load_sem,
    picks_sem,
    send_sem,
    recv_sem,
    wet_send_sem,
    wet_recv_sem,
    ready_sem,
):
    sends, recvs = (send_0, send_1, send_2), (recv_0, recv_1, recv_2)
    groups = len(sends)
    blocks, fields, cells = accum.shape
    core, chip = lax.axis_index("grp"), lax.axis_index("dev")
    me = (core, chip // (SIDE * SIDE), (chip // SIDE) % SIDE, chip % SIDE)
    mine = core * CHIPS + chip

    loads = [
        pltpu.make_async_copy(src, dst, load_sem.at[number])
        for number, (src, dst) in enumerate(
            (
                (slot_hbm, slot),
                (length_hbm, length_ref),
                (accum_hbm, accum),
                (count_hbm, count_smem),
                (wet_hbm, wet_smem),
                (slot_hbm, slot_smem),
            )
        )
    ]
    for load in loads:
        load.start()
    barrier = pltpu.get_barrier_semaphore()

    def greet(other):
        pl.semaphore_signal(barrier, 1, device_id=other, device_id_type=MESH)

    visit_all(STAGES[0], me, greet)

    for load in loads[:2]:
        load.wait()
    row = lax.broadcasted_iota(jnp.int32, (128, 128), 0)
    lane = lax.broadcasted_iota(jnp.int32, (128, 128), 1)
    length = length_ref[...]
    length_col = jnp.sum(jnp.where(row == lane, length, 0), axis=1, keepdims=True)
    end = jnp.sum(jnp.where(row <= lane, length_col, 0), axis=0, keepdims=True)
    start = end - length
    slots = slot[...]
    held = (slots >> 7) == mine
    column = jnp.sum(jnp.where(held, lane, 0), axis=1, keepdims=True)
    local = jnp.sum(jnp.where(held, slots & 127, 0), axis=1, keepdims=True)
    order = row * 128 + column - start
    inside = (order >= 0) & (order < length)
    ahead, behind = order == -1, order == length
    for number, chosen in enumerate((inside & (order < 128), inside & (order >= 128), ahead, behind)):
        picks[number : number + 1, :] = jnp.sum(jnp.where(chosen, local, 0), axis=0, keepdims=True)
    picks_copy = pltpu.make_async_copy(picks, picks_smem, picks_sem)
    picks_copy.start()
    has_ahead = jnp.sum(jnp.where(ahead, 1.0, 0.0), axis=0, keepdims=True)
    has_behind = jnp.sum(jnp.where(behind, 1.0, 0.0), axis=0, keepdims=True)
    at_me = lax.broadcasted_iota(jnp.int32, (1, 128), 1) == mine
    my_start = jnp.sum(jnp.where(at_me, start, 0))
    my_length = jnp.sum(jnp.where(at_me, length, 0))
    final = jnp.maximum(my_length, 1) - 1

    for load in loads[3:5]:
        load.wait()
    at_field = lax.broadcasted_iota(jnp.int32, (GROUP, cells), 0)
    scales = []
    for group in range(groups):
        count = jnp.ones((GROUP, cells), jnp.int32)
        for field in range(GROUP):
            count = jnp.where(at_field == field, count_smem[group * GROUP + field], count)
        scales.append(0.25 / count.astype(jnp.float32))

    def is_wet(index):
        return wet_smem[index >> 7, index & 127] == 1

    wet_send[0] = jnp.full((GROUP, cells), jnp.where(is_wet(final), 1.0, 0.0), jnp.float32)
    wet_send[1] = jnp.full((GROUP, cells), jnp.where(is_wet(0), 1.0, 0.0), jnp.float32)

    picks_copy.wait()
    loads[2].wait()

    def pack(group):
        fields_of = slice(group * GROUP, (group + 1) * GROUP)

        def one(owner, carry):
            for rank in range(2):
                block = accum[picks_smem[rank, owner], fields_of]
                sends[group][owner, rank * GROUP : (rank + 1) * GROUP] = block * scales[group]
            return carry

        lax.fori_loop(0, DEVICES, one, 0, unroll=16)

    def keep_mine(group):
        recvs[group][mine] = sends[group][mine]

    def post(stage):
        group = STAGES[stage][0]

        def to(other):
            pltpu.make_async_remote_copy(
                src_ref=sends[group].at[number_of(other)],
                dst_ref=recvs[group].at[mine],
                send_sem=send_sem.at[stage],
                recv_sem=recv_sem.at[group],
                device_id=other,
                device_id_type=MESH,
            ).start()

        visit_all(STAGES[stage], me, to)

    def sent(stage):
        part = sends[STAGES[stage][0]].at[pl.ds(0, how_many(STAGES[stage]))]
        pltpu.make_async_copy(part, part, send_sem.at[stage]).wait()

    pack(0)
    keep_mine(0)
    pl.semaphore_wait(barrier, how_many(STAGES[0]))
    corners = [steps for steps in itertools.product(range(2), repeat=3) if any(steps)]
    for steps in corners:
        y, x, z = ((at + step) % SIDE for at, step in zip(me[1:], steps))
        pl.semaphore_signal(
            ready_sem, 1, device_id=(core, (y * SIDE + x) * SIDE + z), device_id_type=MESH
        )
    wet_copies = []
    for side, step in enumerate((1, DEVICES - 1)):
        copy = pltpu.make_async_remote_copy(
            src_ref=wet_send.at[side],
            dst_ref=wet_recv.at[side],
            send_sem=wet_send_sem.at[side],
            recv_sem=wet_recv_sem.at[side],
            device_id=device_of((mine + step) % DEVICES),
            device_id_type=MESH,
        )
        copy.start()
        wet_copies.append(copy)
    post(0)
    pl.semaphore_wait(ready_sem, len(corners))
    post(1)

    all_scales = jnp.concatenate(scales, axis=0)
    wide_lane = lax.broadcasted_iota(jnp.int32, (fields, cells), 1)

    def collect(owner, carry):
        cells_ahead, cells_behind = carry
        here = wide_lane == owner
        last = accum[picks_smem[2, owner]][:, cells - 1 : cells]
        first = accum[picks_smem[3, owner]][:, 0:1]
        return jnp.where(here, last, cells_ahead), jnp.where(here, first, cells_behind)

    nothing = jnp.zeros((fields, cells), jnp.float32)
    cells_ahead, cells_behind = lax.fori_loop(0, DEVICES, collect, (nothing, nothing), unroll=8)
    gathered = jnp.concatenate(
        [
            cells_ahead * all_scales * has_ahead,
            cells_behind * all_scales * has_behind,
            jnp.zeros((128 - 2 * fields, cells), jnp.float32),
        ],
        axis=0,
    )
    edge_rows[...] = gathered.T

    def attach(owner, carry):
        sends[EDGE_GROUP][owner, 2 * GROUP : 2 * GROUP + 1] = edge_rows[pl.ds(owner, 1)]
        return carry

    lax.fori_loop(0, DEVICES, attach, 0, unroll=16)
    for group in range(1, groups):
        pack(group)
        keep_mine(group)

    loads[5].wait()

    def table(index, carry):
        block = jnp.minimum(my_start + index, DEVICES * blocks - 1)
        behind_me = index == my_length
        from_smem[index] = jnp.where(behind_me, DEVICES, slot_smem[block >> 7, block & 127] >> 7)
        keep = jnp.where((index < my_length) & is_wet(index), 1.0, 0.0)
        keep_smem[index] = keep
        take_smem[index] = jnp.where(behind_me, 1.0, keep)
        return carry

    capacity = out_ref.shape[0]
    lax.fori_loop(0, capacity, table, 0, unroll=16)
    from_smem[capacity] = DEVICES
    take_smem[capacity] = 1.0

    at_lane = lax.broadcasted_iota(jnp.int32, (GROUP, cells), 1)
    first_lane, last_lane = at_lane == 0, at_lane == cells - 1

    def arrived(group):
        those = recvs[group].at[pl.ds(0, DEVICES - 1)]
        pltpu.make_async_copy(those, those, recv_sem.at[group]).wait()

    def edges():
        def add(sender, carry):
            return carry + recvs[EDGE_GROUP][sender, 2 * GROUP : 2 * GROUP + 1]

        total = lax.fori_loop(0, DEVICES, add, jnp.zeros((1, cells), jnp.float32), unroll=16)
        lefts = []
        for group in range(groups):
            left, right = (
                jnp.sum(jnp.where(at_lane == at_field + side * fields + group * GROUP, total, 0.0), axis=1, keepdims=True)
                for side in range(2)
            )
            lefts.append(left * wet_recv[0])
            for rank in range(2):
                recvs[group][DEVICES, rank * GROUP : (rank + 1) * GROUP] = right * wet_recv[1]
        return lefts

    def smooth(group, left):
        recv = recvs[group]
        fields_of = slice(group * GROUP, (group + 1) * GROUP)

        def value(index, rank):
            return recv[from_smem[index], rank * GROUP : (rank + 1) * GROUP] * take_smem[index]

        def both(block):
            return block, pltpu.roll(block, 1, 1), pltpu.roll(block, cells - 1, 1)

        def one(index, next_rank, carry):
            (current, to_right, to_left), previous = carry
            following = both(value(index + 1, next_rank))
            cell_before = jnp.where(first_lane, previous, to_right)
            cell_after = jnp.where(last_lane, following[2], to_left)
            out_ref[index, fields_of] = ((current + current) + (cell_before + cell_after)) * keep_smem[index]
            return following, to_right

        carry = (both(value(0, 0)), left)
        half = capacity // 2
        for index in range(capacity):
            carry = one(index, 0 if index < half - 1 else 1, carry)

    for stage in range(2):
        sent(stage)
        post(stage + 2)
    arrived(0)
    for stage in range(2, 4):
        sent(stage)
        post(stage + 2)
    arrived(1)
    for copy in wet_copies:
        copy.wait()
    lefts = edges()
    smooth(0, lefts[0])
    smooth(1, lefts[1])
    arrived(2)
    smooth(2, lefts[2])
    sent(4)
    sent(5)


def on_device(accum, step_count, stretch_slot, span_length, wet_mask):
    blocks, fields, cells = accum.shape
    capacity = wet_mask.shape[0]
    groups = fields // GROUP
    heights = [2 * GROUP + (group == EDGE_GROUP) for group in range(groups)]
    arguments = (
        accum,
        stretch_slot.reshape(-1, 128),
        span_length.reshape(1, -1),
        wet_mask.reshape(-1, 128),
        step_count,
    )
    return pl.pallas_call(
        kernel,
        out_shape=pltpu.VMEM((capacity, fields, cells), jnp.float32),
        in_specs=[pl.BlockSpec(memory_space=pltpu.HBM)] * len(arguments),
        out_specs=pl.BlockSpec(memory_space=pltpu.VMEM),
        scratch_shapes=[
            pltpu.VMEM((blocks, fields, cells), jnp.float32),
            pltpu.VMEM((128, 128), jnp.int32),
            pltpu.VMEM((1, 128), jnp.int32),
            *[pltpu.VMEM((DEVICES, height, cells), jnp.float32) for height in heights],
            *[pltpu.VMEM((DEVICES + 1, height, cells), jnp.float32) for height in heights],
            pltpu.VMEM((128, cells), jnp.float32),
            pltpu.VMEM((2, GROUP, cells), jnp.float32),
            pltpu.VMEM((2, GROUP, cells), jnp.float32),
            pltpu.VMEM((4, 128), jnp.int32),
            pltpu.SMEM((4, 128), jnp.int32),
            pltpu.SMEM((128, 128), jnp.int32),
            pltpu.SMEM((capacity // 128, 128), jnp.int32),
            pltpu.SMEM((fields,), jnp.int32),
            pltpu.SMEM((capacity + 1,), jnp.int32),
            pltpu.SMEM((capacity + 1,), jnp.float32),
            pltpu.SMEM((capacity,), jnp.float32),
            pltpu.SemaphoreType.DMA((6,)),
            pltpu.SemaphoreType.DMA,
            pltpu.SemaphoreType.DMA((2 * groups,)),
            pltpu.SemaphoreType.DMA((groups,)),
            pltpu.SemaphoreType.DMA((2,)),
            pltpu.SemaphoreType.DMA((2,)),
            pltpu.SemaphoreType.REGULAR,
        ],
        compiler_params=pltpu.CompilerParams(
            collective_id=0, has_side_effects=True, vmem_limit_bytes=32 * 1024 * 1024
        ),
        name="remap",
    )(*(pltpu.with_memory_space_constraint(a, pltpu.HBM) for a in arguments))


def solution(mesh):
    return jax.shard_map(
        on_device,
        mesh=mesh,
        in_specs=(P(("grp", "dev"), None, None), P(), P(), P(), P(("grp", "dev"))),
        out_specs=P(("grp", "dev"), None, None),
        check_vma=False,
    )
```

```python
import functools
import itertools

import jax
import jax.numpy as jnp
from jax import lax
from jax.experimental import pallas as pl
from jax.experimental.pallas import tpu as pltpu
from jax.sharding import PartitionSpec as P

MESH = pl.DeviceIdType.MESH
SIDE = 4
CHIPS = SIDE**3
DEVICES = 2 * CHIPS
GROUP = 8
EDGE_GROUP = 1

STEPS = sorted(
    itertools.product(range(SIDE), repeat=3),
    key=lambda steps: (2 not in steps, -sum(min(step, SIDE - step) for step in steps)),
)
FAR = sum(2 in steps for steps in STEPS)
PACKED = [
    sum((STEPS[at + k][0] * 16 + STEPS[at + k][1] * 4 + STEPS[at + k][2]) << (6 * k) for k in range(4))
    for at in range(0, CHIPS, 4)
]
STAGES = [(0, (FAR, CHIPS), (0, 1)), (0, (0, FAR), (0, 1))] + [
    (group, (0, CHIPS), (turn,)) for group in (1, 2) for turn in range(2)
]


def how_many(stage):
    _, (low, high), turns = stage
    return sum(high - low - (turn == 0 and high == CHIPS) for turn in turns)


def visit_all(stage, me, visit):
    _, (low, high), turns = stage
    core, y, x, z = me

    def one(index, carry):
        number = PACKED[0]
        for k, packed in enumerate(PACKED[1:], 1):
            number = jnp.where(index >> 2 == k, packed, number)
        number = number >> (6 * (index & 3))
        chip = (((y + (number >> 4)) & 3) * SIDE + ((x + (number >> 2)) & 3)) * SIDE + ((z + number) & 3)
        for turn in turns:
            visit(((core + turn) & 1, chip))
        return carry

    if len(turns) == 1:
        lax.fori_loop(low, min(high, CHIPS - (turns[0] == 0)), one, 0)
        return
    lax.fori_loop(low, min(high, CHIPS - 1), one, 0)
    if high == CHIPS:
        visit(((core + 1) & 1, (y * SIDE + x) * SIDE + z))


def number_of(device):
    return device[0] * CHIPS + device[1]


def device_of(number):
    return number // CHIPS, number % CHIPS


def smooth(recv, out, first_field, left, tables, slots, carry=None):
    from_smem, take_smem, keep_smem = tables
    capacity, cells = out.shape[0], out.shape[2]
    at_lane = lax.broadcasted_iota(jnp.int32, (GROUP, cells), 1)
    first_lane, last_lane = at_lane == 0, at_lane == cells - 1

    def both(index):
        rank = int(index >= capacity // 2)
        block = recv[from_smem[index], rank * GROUP : (rank + 1) * GROUP] * take_smem[index]
        return block, pltpu.roll(block, 1, 1), pltpu.roll(block, cells - 1, 1)

    if carry is None:
        carry = both(0), left
    for index in slots:
        (current, to_right, to_left), previous = carry
        following = both(index + 1)
        cell_before = jnp.where(first_lane, previous, to_right)
        cell_after = jnp.where(last_lane, following[2], to_left)
        smoothed = ((current + current) + (cell_before + cell_after)) * keep_smem[index]
        out[index, first_field : first_field + GROUP] = smoothed
        carry = following, to_right
    return carry


def finish(parts, done, recv, left, from_smem, take_smem, keep_smem, out_hbm, last, done_sem, last_sem):
    capacity, ready, _ = done.shape
    rows = capacity // parts
    whole = [
        pltpu.make_async_copy(
            done.at[pl.ds(part * rows, rows)],
            out_hbm.at[pl.ds(part * rows, rows), pl.ds(0, ready)],
            done_sem.at[part],
        )
        for part in range(parts)
    ]
    for copy in whole:
        copy.start()
    carry, rest = None, []
    for part in range(parts):
        slots = range(part * rows, (part + 1) * rows)
        carry = smooth(recv, last, 0, left[...], (from_smem, take_smem, keep_smem), slots, carry)
        copy = pltpu.make_async_copy(
            last.at[pl.ds(part * rows, rows)],
            out_hbm.at[pl.ds(part * rows, rows), pl.ds(ready, GROUP)],
            last_sem.at[part],
        )
        copy.start()
        rest.append(copy)
    for copy in whole + rest:
        copy.wait()


def kernel(
    accum_hbm,
    slot_hbm,
    length_hbm,
    wet_hbm,
    count_hbm,
    out_ref,
    recv_2,
    left_ref,
    from_smem,
    take_smem,
    keep_smem,
    accum,
    slot,
    length_ref,
    send_0,
    send_1,
    send_2,
    recv_0,
    recv_1,
    edge_rows,
    wet_send,
    wet_recv,
    picks,
    picks_smem,
    slot_smem,
    wet_smem,
    count_smem,
    load_sem,
    picks_sem,
    send_sem,
    recv_sem,
    wet_send_sem,
    wet_recv_sem,
    ready_sem,
):
    sends, recvs = (send_0, send_1, send_2), (recv_0, recv_1, recv_2)
    groups = len(sends)
    blocks, fields, cells = accum.shape
    core, chip = lax.axis_index("grp"), lax.axis_index("dev")
    me = (core, chip // (SIDE * SIDE), (chip // SIDE) % SIDE, chip % SIDE)
    mine = core * CHIPS + chip

    loads = [
        pltpu.make_async_copy(src, dst, load_sem.at[number])
        for number, (src, dst) in enumerate(
            (
                (slot_hbm, slot),
                (length_hbm, length_ref),
                (accum_hbm, accum),
                (count_hbm, count_smem),
                (wet_hbm, wet_smem),
                (slot_hbm, slot_smem),
            )
        )
    ]
    for load in loads:
        load.start()
    barrier = pltpu.get_barrier_semaphore()

    def greet(other):
        pl.semaphore_signal(barrier, 1, device_id=other, device_id_type=MESH)

    visit_all(STAGES[0], me, greet)

    for load in loads[:2]:
        load.wait()
    row = lax.broadcasted_iota(jnp.int32, (128, 128), 0)
    lane = lax.broadcasted_iota(jnp.int32, (128, 128), 1)
    length = length_ref[...]
    length_col = jnp.sum(jnp.where(row == lane, length, 0), axis=1, keepdims=True)
    end = jnp.sum(jnp.where(row <= lane, length_col, 0), axis=0, keepdims=True)
    start = end - length
    slots = slot[...]
    held = (slots >> 7) == mine
    column = jnp.sum(jnp.where(held, lane, 0), axis=1, keepdims=True)
    local = jnp.sum(jnp.where(held, slots & 127, 0), axis=1, keepdims=True)
    order = row * 128 + column - start
    inside = (order >= 0) & (order < length)
    ahead, behind = order == -1, order == length
    for number, chosen in enumerate((inside & (order < 128), inside & (order >= 128), ahead, behind)):
        picks[number : number + 1, :] = jnp.sum(jnp.where(chosen, local, 0), axis=0, keepdims=True)
    picks_copy = pltpu.make_async_copy(picks, picks_smem, picks_sem)
    picks_copy.start()
    has_ahead = jnp.sum(jnp.where(ahead, 1.0, 0.0), axis=0, keepdims=True)
    has_behind = jnp.sum(jnp.where(behind, 1.0, 0.0), axis=0, keepdims=True)
    at_me = lax.broadcasted_iota(jnp.int32, (1, 128), 1) == mine
    my_start = jnp.sum(jnp.where(at_me, start, 0))
    my_length = jnp.sum(jnp.where(at_me, length, 0))
    final = jnp.maximum(my_length, 1) - 1

    for load in loads[3:5]:
        load.wait()
    at_field = lax.broadcasted_iota(jnp.int32, (GROUP, cells), 0)
    scales = []
    for group in range(groups):
        count = jnp.ones((GROUP, cells), jnp.int32)
        for field in range(GROUP):
            count = jnp.where(at_field == field, count_smem[group * GROUP + field], count)
        scales.append(0.25 / count.astype(jnp.float32))

    def is_wet(index):
        return wet_smem[index >> 7, index & 127] == 1

    wet_send[0] = jnp.full((GROUP, cells), jnp.where(is_wet(final), 1.0, 0.0), jnp.float32)
    wet_send[1] = jnp.full((GROUP, cells), jnp.where(is_wet(0), 1.0, 0.0), jnp.float32)

    picks_copy.wait()
    loads[2].wait()

    def pack(group):
        fields_of = slice(group * GROUP, (group + 1) * GROUP)

        def one(owner, carry):
            for rank in range(2):
                block = accum[picks_smem[rank, owner], fields_of]
                sends[group][owner, rank * GROUP : (rank + 1) * GROUP] = block * scales[group]
            return carry

        lax.fori_loop(0, DEVICES, one, 0, unroll=16)

    def keep_mine(group):
        recvs[group][mine] = sends[group][mine]

    def post(stage):
        group = STAGES[stage][0]

        def to(other):
            pltpu.make_async_remote_copy(
                src_ref=sends[group].at[number_of(other)],
                dst_ref=recvs[group].at[mine],
                send_sem=send_sem.at[stage],
                recv_sem=recv_sem.at[group],
                device_id=other,
                device_id_type=MESH,
            ).start()

        visit_all(STAGES[stage], me, to)

    def sent(stage):
        part = sends[STAGES[stage][0]].at[pl.ds(0, how_many(STAGES[stage]))]
        pltpu.make_async_copy(part, part, send_sem.at[stage]).wait()

    pack(0)
    keep_mine(0)
    pl.semaphore_wait(barrier, how_many(STAGES[0]))
    corners = [steps for steps in itertools.product(range(2), repeat=3) if any(steps)]
    for steps in corners:
        y, x, z = ((at + step) % SIDE for at, step in zip(me[1:], steps))
        pl.semaphore_signal(
            ready_sem, 1, device_id=(core, (y * SIDE + x) * SIDE + z), device_id_type=MESH
        )
    wet_copies = []
    for side, step in enumerate((1, DEVICES - 1)):
        copy = pltpu.make_async_remote_copy(
            src_ref=wet_send.at[side],
            dst_ref=wet_recv.at[side],
            send_sem=wet_send_sem.at[side],
            recv_sem=wet_recv_sem.at[side],
            device_id=device_of((mine + step) % DEVICES),
            device_id_type=MESH,
        )
        copy.start()
        wet_copies.append(copy)
    post(0)
    pl.semaphore_wait(ready_sem, len(corners))
    post(1)

    all_scales = jnp.concatenate(scales, axis=0)
    wide_lane = lax.broadcasted_iota(jnp.int32, (fields, cells), 1)

    def collect(owner, carry):
        cells_ahead, cells_behind = carry
        here = wide_lane == owner
        last = accum[picks_smem[2, owner]][:, cells - 1 : cells]
        first = accum[picks_smem[3, owner]][:, 0:1]
        return jnp.where(here, last, cells_ahead), jnp.where(here, first, cells_behind)

    nothing = jnp.zeros((fields, cells), jnp.float32)
    cells_ahead, cells_behind = lax.fori_loop(0, DEVICES, collect, (nothing, nothing), unroll=8)
    gathered = jnp.concatenate(
        [
            cells_ahead * all_scales * has_ahead,
            cells_behind * all_scales * has_behind,
            jnp.zeros((128 - 2 * fields, cells), jnp.float32),
        ],
        axis=0,
    )
    edge_rows[...] = gathered.T

    def attach(owner, carry):
        sends[EDGE_GROUP][owner, 2 * GROUP : 2 * GROUP + 1] = edge_rows[pl.ds(owner, 1)]
        return carry

    lax.fori_loop(0, DEVICES, attach, 0, unroll=16)
    for group in range(1, groups):
        pack(group)
        keep_mine(group)

    loads[5].wait()

    def table(index, carry):
        block = jnp.minimum(my_start + index, DEVICES * blocks - 1)
        behind_me = index == my_length
        from_smem[index] = jnp.where(behind_me, DEVICES, slot_smem[block >> 7, block & 127] >> 7)
        keep = jnp.where((index < my_length) & is_wet(index), 1.0, 0.0)
        keep_smem[index] = keep
        take_smem[index] = jnp.where(behind_me, 1.0, keep)
        return carry

    capacity = out_ref.shape[0]
    lax.fori_loop(0, capacity, table, 0, unroll=16)
    from_smem[capacity] = DEVICES
    take_smem[capacity] = 1.0

    at_lane = lax.broadcasted_iota(jnp.int32, (GROUP, cells), 1)
    first_lane, last_lane = at_lane == 0, at_lane == cells - 1

    def arrived(group):
        those = recvs[group].at[pl.ds(0, DEVICES - 1)]
        pltpu.make_async_copy(those, those, recv_sem.at[group]).wait()

    def edges():
        def add(sender, carry):
            return carry + recvs[EDGE_GROUP][sender, 2 * GROUP : 2 * GROUP + 1]

        total = lax.fori_loop(0, DEVICES, add, jnp.zeros((1, cells), jnp.float32), unroll=16)
        lefts = []
        for group in range(groups):
            left, right = (
                jnp.sum(jnp.where(at_lane == at_field + side * fields + group * GROUP, total, 0.0), axis=1, keepdims=True)
                for side in range(2)
            )
            lefts.append(left * wet_recv[0])
            for rank in range(2):
                recvs[group][DEVICES, rank * GROUP : (rank + 1) * GROUP] = right * wet_recv[1]
        return lefts

    for stage in range(2):
        sent(stage)
        post(stage + 2)
    arrived(0)
    for stage in range(2, 4):
        sent(stage)
        post(stage + 2)
    arrived(1)
    for copy in wet_copies:
        copy.wait()
    lefts = edges()
    for group in range(2):
        tables = from_smem, take_smem, keep_smem
        smooth(recvs[group], out_ref, group * GROUP, lefts[group], tables, range(capacity))
    left_ref[...] = jnp.broadcast_to(lefts[2], left_ref.shape)
    arrived(2)
    sent(4)
    sent(5)


def on_device(accum, step_count, stretch_slot, span_length, wet_mask):
    blocks, fields, cells = accum.shape
    capacity = wet_mask.shape[0]
    groups = fields // GROUP
    heights = [2 * GROUP + (group == EDGE_GROUP) for group in range(groups)]
    arguments = (
        accum,
        stretch_slot.reshape(-1, 128),
        span_length.reshape(1, -1),
        wet_mask.reshape(-1, 128),
        step_count,
    )
    outcome = pl.pallas_call(
        kernel,
        out_shape=(
            pltpu.VMEM((capacity, fields - GROUP, cells), jnp.float32),
            pltpu.VMEM((DEVICES + 1, heights[2], cells), jnp.float32),
            pltpu.VMEM((GROUP, cells), jnp.float32),
            pltpu.SMEM((capacity + 1,), jnp.int32),
            pltpu.SMEM((capacity + 1,), jnp.float32),
            pltpu.SMEM((capacity,), jnp.float32),
        ),
        in_specs=[pl.BlockSpec(memory_space=pltpu.HBM)] * len(arguments),
        out_specs=[pl.BlockSpec(memory_space=pltpu.VMEM)] * 3 + [pl.BlockSpec(memory_space=pltpu.SMEM)] * 3,
        scratch_shapes=[
            pltpu.VMEM((blocks, fields, cells), jnp.float32),
            pltpu.VMEM((128, 128), jnp.int32),
            pltpu.VMEM((1, 128), jnp.int32),
            *[pltpu.VMEM((DEVICES, height, cells), jnp.float32) for height in heights],
            *[pltpu.VMEM((DEVICES + 1, height, cells), jnp.float32) for height in heights[:2]],
            pltpu.VMEM((128, cells), jnp.float32),
            pltpu.VMEM((2, GROUP, cells), jnp.float32),
            pltpu.VMEM((2, GROUP, cells), jnp.float32),
            pltpu.VMEM((4, 128), jnp.int32),
            pltpu.SMEM((4, 128), jnp.int32),
            pltpu.SMEM((128, 128), jnp.int32),
            pltpu.SMEM((capacity // 128, 128), jnp.int32),
            pltpu.SMEM((fields,), jnp.int32),
            pltpu.SemaphoreType.DMA((6,)),
            pltpu.SemaphoreType.DMA,
            pltpu.SemaphoreType.DMA((2 * groups,)),
            pltpu.SemaphoreType.DMA((groups,)),
            pltpu.SemaphoreType.DMA((2,)),
            pltpu.SemaphoreType.DMA((2,)),
            pltpu.SemaphoreType.REGULAR,
        ],
        compiler_params=pltpu.CompilerParams(
            collective_id=0, has_side_effects=True, vmem_limit_bytes=32 * 1024 * 1024
        ),
        name="remap",
    )(*(pltpu.with_memory_space_constraint(a, pltpu.HBM) for a in arguments))

    parts = 4
    return pl.pallas_call(
        functools.partial(finish, parts),
        out_shape=pltpu.HBM((capacity, fields, cells), jnp.float32),
        in_specs=[pl.BlockSpec(memory_space=pltpu.VMEM)] * 3 + [pl.BlockSpec(memory_space=pltpu.SMEM)] * 3,
        out_specs=pl.BlockSpec(memory_space=pltpu.HBM),
        scratch_shapes=[
            pltpu.VMEM((capacity, GROUP, cells), jnp.float32),
            pltpu.SemaphoreType.DMA((parts,)),
            pltpu.SemaphoreType.DMA((parts,)),
        ],
        compiler_params=pltpu.CompilerParams(vmem_limit_bytes=16 * 1024 * 1024),
        name="finish",
    )(
        *(pltpu.with_memory_space_constraint(a, pltpu.VMEM) for a in outcome[:3]),
        *(pltpu.with_memory_space_constraint(a, pltpu.SMEM) for a in outcome[3:]),
    )


def solution(mesh):
    return jax.shard_map(
        on_device,
        mesh=mesh,
        in_specs=(P(("grp", "dev"), None, None), P(), P(), P(), P(("grp", "dev"))),
        out_specs=P(("grp", "dev"), None, None),
        check_vma=False,
    )
```

```python
import functools
import itertools

import jax
import jax.numpy as jnp
from jax import lax
from jax.experimental import pallas as pl
from jax.experimental.pallas import tpu as pltpu
from jax.sharding import PartitionSpec as P

MESH = pl.DeviceIdType.MESH
SIDE = 4
CHIPS = SIDE**3
DEVICES = 2 * CHIPS
GROUP = 8
EDGE_GROUP = 1

STEPS = sorted(
    itertools.product(range(SIDE), repeat=3),
    key=lambda steps: (2 not in steps, -sum(min(step, SIDE - step) for step in steps)),
)
FAR = sum(2 in steps for steps in STEPS)
PACKED = [
    sum((STEPS[at + k][0] * 16 + STEPS[at + k][1] * 4 + STEPS[at + k][2]) << (6 * k) for k in range(4))
    for at in range(0, CHIPS, 4)
]
STAGES = [(0, (FAR, CHIPS), (0, 1)), (0, (0, FAR), (0, 1))] + [
    (group, (0, CHIPS), (turn,)) for group in (1, 2) for turn in range(2)
]


def how_many(stage):
    _, (low, high), turns = stage
    return sum(high - low - (turn == 0 and high == CHIPS) for turn in turns)


def visit_all(stage, me, visit):
    _, (low, high), turns = stage
    core, y, x, z = me

    def one(index, carry):
        number = PACKED[0]
        for k, packed in enumerate(PACKED[1:], 1):
            number = jnp.where(index >> 2 == k, packed, number)
        number = number >> (6 * (index & 3))
        chip = (((y + (number >> 4)) & 3) * SIDE + ((x + (number >> 2)) & 3)) * SIDE + ((z + number) & 3)
        for turn in turns:
            visit(((core + turn) & 1, chip))
        return carry

    if len(turns) == 1:
        lax.fori_loop(low, min(high, CHIPS - (turns[0] == 0)), one, 0)
        return
    lax.fori_loop(low, min(high, CHIPS - 1), one, 0)
    if high == CHIPS:
        visit(((core + 1) & 1, (y * SIDE + x) * SIDE + z))


def number_of(device):
    return device[0] * CHIPS + device[1]


def device_of(number):
    return number // CHIPS, number % CHIPS


def smooth(recv, out, first_field, left, tables, slots, carry=None):
    from_smem, take_smem, keep_smem = tables
    capacity, cells = out.shape[0], out.shape[2]
    at_lane = lax.broadcasted_iota(jnp.int32, (GROUP, cells), 1)
    first_lane, last_lane = at_lane == 0, at_lane == cells - 1

    def both(index):
        rank = int(index >= capacity // 2)
        block = recv[from_smem[index], rank * GROUP : (rank + 1) * GROUP] * take_smem[index]
        return block, pltpu.roll(block, 1, 1), pltpu.roll(block, cells - 1, 1)

    if carry is None:
        carry = both(0), left
    for index in slots:
        (current, to_right, to_left), previous = carry
        following = both(index + 1)
        cell_before = jnp.where(first_lane, previous, to_right)
        cell_after = jnp.where(last_lane, following[2], to_left)
        smoothed = ((current + current) + (cell_before + cell_after)) * keep_smem[index]
        out[index, first_field : first_field + GROUP] = smoothed
        carry = following, to_right
    return carry


def finish(parts, done, recv, left, from_smem, take_smem, keep_smem, out_hbm, last, done_sem, last_sem):
    capacity, ready, _ = done.shape
    rows = capacity // parts
    whole = [
        pltpu.make_async_copy(
            done.at[pl.ds(part * rows, rows)],
            out_hbm.at[pl.ds(part * rows, rows), pl.ds(0, ready)],
            done_sem.at[part],
        )
        for part in range(parts)
    ]
    for copy in whole:
        copy.start()
    carry, rest = None, []
    for part in range(parts):
        slots = range(part * rows, (part + 1) * rows)
        carry = smooth(recv, last, 0, left[...], (from_smem, take_smem, keep_smem), slots, carry)
        copy = pltpu.make_async_copy(
            last.at[pl.ds(part * rows, rows)],
            out_hbm.at[pl.ds(part * rows, rows), pl.ds(ready, GROUP)],
            last_sem.at[part],
        )
        copy.start()
        rest.append(copy)
    for copy in whole + rest:
        copy.wait()


def kernel(
    accum_hbm,
    slot_hbm,
    length_hbm,
    wet_hbm,
    count_hbm,
    out_ref,
    recv_2,
    left_ref,
    from_smem,
    take_smem,
    keep_smem,
    accum,
    slot,
    length_ref,
    send_0,
    send_1,
    send_2,
    recv_0,
    recv_1,
    edge_rows,
    wet_send,
    wet_recv,
    picks,
    picks_smem,
    slot_smem,
    wet_smem,
    count_smem,
    load_sem,
    picks_sem,
    send_sem,
    recv_sem,
    wet_send_sem,
    wet_recv_sem,
    ready_sem,
):
    sends, recvs = (send_0, send_1, send_2), (recv_0, recv_1, recv_2)
    groups = len(sends)
    blocks, fields, cells = accum.shape
    core, chip = lax.axis_index("grp"), lax.axis_index("dev")
    me = (core, chip // (SIDE * SIDE), (chip // SIDE) % SIDE, chip % SIDE)
    mine = core * CHIPS + chip

    loads = [
        pltpu.make_async_copy(src, dst, load_sem.at[number])
        for number, (src, dst) in enumerate(
            (
                (slot_hbm, slot),
                (length_hbm, length_ref),
                (accum_hbm, accum),
                (count_hbm, count_smem),
                (wet_hbm, wet_smem),
                (slot_hbm, slot_smem),
            )
        )
    ]
    for load in loads:
        load.start()
    barrier = pltpu.get_barrier_semaphore()

    def greet(other):
        pl.semaphore_signal(barrier, 1, device_id=other, device_id_type=MESH)

    visit_all(STAGES[0], me, greet)

    for load in loads[:2]:
        load.wait()
    row = lax.broadcasted_iota(jnp.int32, (128, 128), 0)
    lane = lax.broadcasted_iota(jnp.int32, (128, 128), 1)
    length = length_ref[...]
    length_col = jnp.sum(jnp.where(row == lane, length, 0), axis=1, keepdims=True)
    end = jnp.sum(jnp.where(row <= lane, length_col, 0), axis=0, keepdims=True)
    start = end - length
    slots = slot[...]
    held = (slots >> 7) == mine
    column = jnp.sum(jnp.where(held, lane, 0), axis=1, keepdims=True)
    local = jnp.sum(jnp.where(held, slots & 127, 0), axis=1, keepdims=True)
    order = row * 128 + column - start
    inside = (order >= 0) & (order < length)
    ahead, behind = order == -1, order == length
    for number, chosen in enumerate((inside & (order < 128), inside & (order >= 128), ahead, behind)):
        picks[number : number + 1, :] = jnp.sum(jnp.where(chosen, local, 0), axis=0, keepdims=True)
    picks_copy = pltpu.make_async_copy(picks, picks_smem, picks_sem)
    picks_copy.start()
    has_ahead = jnp.sum(jnp.where(ahead, 1.0, 0.0), axis=0, keepdims=True)
    has_behind = jnp.sum(jnp.where(behind, 1.0, 0.0), axis=0, keepdims=True)
    at_me = lax.broadcasted_iota(jnp.int32, (1, 128), 1) == mine
    my_start = jnp.sum(jnp.where(at_me, start, 0))
    my_length = jnp.sum(jnp.where(at_me, length, 0))
    final = jnp.maximum(my_length, 1) - 1

    for load in loads[3:5]:
        load.wait()
    at_field = lax.broadcasted_iota(jnp.int32, (GROUP, cells), 0)
    scales = []
    for group in range(groups):
        count = jnp.ones((GROUP, cells), jnp.int32)
        for field in range(GROUP):
            count = jnp.where(at_field == field, count_smem[group * GROUP + field], count)
        scales.append(0.25 / count.astype(jnp.float32))

    def is_wet(index):
        return wet_smem[index >> 7, index & 127] == 1

    wet_send[0] = jnp.full((GROUP, cells), jnp.where(is_wet(final), 1.0, 0.0), jnp.float32)
    wet_send[1] = jnp.full((GROUP, cells), jnp.where(is_wet(0), 1.0, 0.0), jnp.float32)

    picks_copy.wait()
    loads[2].wait()

    def pack(group):
        fields_of = slice(group * GROUP, (group + 1) * GROUP)

        def one(owner, carry):
            for rank in range(2):
                block = accum[picks_smem[rank, owner], fields_of]
                sends[group][owner, rank * GROUP : (rank + 1) * GROUP] = block * scales[group]
            return carry

        lax.fori_loop(0, DEVICES, one, 0, unroll=16)

    def keep_mine(group):
        recvs[group][mine] = sends[group][mine]

    def post(stage):
        group = STAGES[stage][0]

        def to(other):
            pltpu.make_async_remote_copy(
                src_ref=sends[group].at[number_of(other)],
                dst_ref=recvs[group].at[mine],
                send_sem=send_sem.at[stage],
                recv_sem=recv_sem.at[group],
                device_id=other,
                device_id_type=MESH,
            ).start()

        visit_all(STAGES[stage], me, to)

    def sent(stage):
        part = sends[STAGES[stage][0]].at[pl.ds(0, how_many(STAGES[stage]))]
        pltpu.make_async_copy(part, part, send_sem.at[stage]).wait()

    pack(0)
    keep_mine(0)
    pl.semaphore_wait(barrier, how_many(STAGES[0]))
    corners = [steps for steps in itertools.product(range(2), repeat=3) if any(steps)]
    for steps in corners:
        y, x, z = ((at + step) % SIDE for at, step in zip(me[1:], steps))
        pl.semaphore_signal(
            ready_sem, 1, device_id=(core, (y * SIDE + x) * SIDE + z), device_id_type=MESH
        )
    wet_copies = []
    for side, step in enumerate((1, DEVICES - 1)):
        copy = pltpu.make_async_remote_copy(
            src_ref=wet_send.at[side],
            dst_ref=wet_recv.at[side],
            send_sem=wet_send_sem.at[side],
            recv_sem=wet_recv_sem.at[side],
            device_id=device_of((mine + step) % DEVICES),
            device_id_type=MESH,
        )
        copy.start()
        wet_copies.append(copy)
    post(0)
    pl.semaphore_wait(ready_sem, len(corners))
    post(1)

    all_scales = jnp.concatenate(scales, axis=0)
    wide_lane = lax.broadcasted_iota(jnp.int32, (fields, cells), 1)

    def collect(owner, carry):
        cells_ahead, cells_behind = carry
        here = wide_lane == owner
        last = accum[picks_smem[2, owner]][:, cells - 1 : cells]
        first = accum[picks_smem[3, owner]][:, 0:1]
        return jnp.where(here, last, cells_ahead), jnp.where(here, first, cells_behind)

    nothing = jnp.zeros((fields, cells), jnp.float32)
    cells_ahead, cells_behind = lax.fori_loop(0, DEVICES, collect, (nothing, nothing), unroll=8)
    gathered = jnp.concatenate(
        [
            cells_ahead * all_scales * has_ahead,
            cells_behind * all_scales * has_behind,
            jnp.zeros((128 - 2 * fields, cells), jnp.float32),
        ],
        axis=0,
    )
    edge_rows[...] = gathered.T

    def attach(owner, carry):
        sends[EDGE_GROUP][owner, 2 * GROUP : 2 * GROUP + 1] = edge_rows[pl.ds(owner, 1)]
        return carry

    lax.fori_loop(0, DEVICES, attach, 0, unroll=16)
    for group in range(1, groups):
        pack(group)
        keep_mine(group)

    loads[5].wait()

    def table(index, carry):
        block = jnp.minimum(my_start + index, DEVICES * blocks - 1)
        behind_me = index == my_length
        from_smem[index] = jnp.where(behind_me, DEVICES, slot_smem[block >> 7, block & 127] >> 7)
        keep = jnp.where((index < my_length) & is_wet(index), 1.0, 0.0)
        keep_smem[index] = keep
        take_smem[index] = jnp.where(behind_me, 1.0, keep)
        return carry

    capacity = out_ref.shape[0]
    lax.fori_loop(0, capacity, table, 0, unroll=16)
    from_smem[capacity] = DEVICES
    take_smem[capacity] = 1.0

    at_lane = lax.broadcasted_iota(jnp.int32, (GROUP, cells), 1)
    first_lane, last_lane = at_lane == 0, at_lane == cells - 1

    def arrived(group):
        those = recvs[group].at[pl.ds(0, DEVICES - 1)]
        pltpu.make_async_copy(those, those, recv_sem.at[group]).wait()

    def edges():
        def add(sender, carry):
            return carry + recvs[EDGE_GROUP][sender, 2 * GROUP : 2 * GROUP + 1]

        total = lax.fori_loop(0, DEVICES, add, jnp.zeros((1, cells), jnp.float32), unroll=16)
        lefts = []
        for group in range(groups):
            left, right = (
                jnp.sum(jnp.where(at_lane == at_field + side * fields + group * GROUP, total, 0.0), axis=1, keepdims=True)
                for side in range(2)
            )
            lefts.append(left * wet_recv[0])
            for rank in range(2):
                recvs[group][DEVICES, rank * GROUP : (rank + 1) * GROUP] = right * wet_recv[1]
        return lefts

    for stage in range(2):
        sent(stage)
        post(stage + 2)
    arrived(0)
    for stage in range(2, 4):
        sent(stage)
        post(stage + 2)
    arrived(1)
    for copy in wet_copies:
        copy.wait()
    lefts = edges()
    for group in range(2):
        tables = from_smem, take_smem, keep_smem
        smooth(recvs[group], out_ref, group * GROUP, lefts[group], tables, range(capacity))
    left_ref[...] = jnp.broadcast_to(lefts[2], left_ref.shape)
    arrived(2)
    sent(4)
    sent(5)


def on_device(accum, step_count, stretch_slot, span_length, wet_mask):
    blocks, fields, cells = accum.shape
    capacity = wet_mask.shape[0]
    groups = fields // GROUP
    heights = [2 * GROUP + (group == EDGE_GROUP) for group in range(groups)]
    arguments = (
        accum,
        stretch_slot.reshape(-1, 128),
        span_length.reshape(1, -1),
        wet_mask.reshape(-1, 128),
        step_count,
    )
    outcome = pl.pallas_call(
        kernel,
        out_shape=(
            pltpu.VMEM((capacity, fields - GROUP, cells), jnp.float32),
            pltpu.VMEM((DEVICES + 1, heights[2], cells), jnp.float32),
            pltpu.VMEM((GROUP, cells), jnp.float32),
            pltpu.SMEM((capacity + 1,), jnp.int32),
            pltpu.SMEM((capacity + 1,), jnp.float32),
            pltpu.SMEM((capacity,), jnp.float32),
        ),
        in_specs=[pl.BlockSpec(memory_space=pltpu.HBM)] * len(arguments),
        out_specs=[pl.BlockSpec(memory_space=pltpu.VMEM)] * 3 + [pl.BlockSpec(memory_space=pltpu.SMEM)] * 3,
        scratch_shapes=[
            pltpu.VMEM((blocks, fields, cells), jnp.float32),
            pltpu.VMEM((128, 128), jnp.int32),
            pltpu.VMEM((1, 128), jnp.int32),
            *[pltpu.VMEM((DEVICES, height, cells), jnp.float32) for height in heights],
            *[pltpu.VMEM((DEVICES + 1, height, cells), jnp.float32) for height in heights[:2]],
            pltpu.VMEM((128, cells), jnp.float32),
            pltpu.VMEM((2, GROUP, cells), jnp.float32),
            pltpu.VMEM((2, GROUP, cells), jnp.float32),
            pltpu.VMEM((4, 128), jnp.int32),
            pltpu.SMEM((4, 128), jnp.int32),
            pltpu.SMEM((128, 128), jnp.int32),
            pltpu.SMEM((capacity // 128, 128), jnp.int32),
            pltpu.SMEM((fields,), jnp.int32),
            pltpu.SemaphoreType.DMA((6,)),
            pltpu.SemaphoreType.DMA,
            pltpu.SemaphoreType.DMA((2 * groups,)),
            pltpu.SemaphoreType.DMA((groups,)),
            pltpu.SemaphoreType.DMA((2,)),
            pltpu.SemaphoreType.DMA((2,)),
            pltpu.SemaphoreType.REGULAR,
        ],
        compiler_params=pltpu.CompilerParams(
            collective_id=0, has_side_effects=True, vmem_limit_bytes=32 * 1024 * 1024
        ),
        name="remap",
    )(*(pltpu.with_memory_space_constraint(a, pltpu.HBM) for a in arguments))

    parts = 8
    return pl.pallas_call(
        functools.partial(finish, parts),
        out_shape=pltpu.HBM((capacity, fields, cells), jnp.float32),
        in_specs=[pl.BlockSpec(memory_space=pltpu.VMEM)] * 3 + [pl.BlockSpec(memory_space=pltpu.SMEM)] * 3,
        out_specs=pl.BlockSpec(memory_space=pltpu.HBM),
        scratch_shapes=[
            pltpu.VMEM((capacity, GROUP, cells), jnp.float32),
            pltpu.SemaphoreType.DMA((parts,)),
            pltpu.SemaphoreType.DMA((parts,)),
        ],
        compiler_params=pltpu.CompilerParams(vmem_limit_bytes=16 * 1024 * 1024),
        name="finish",
    )(
        *(pltpu.with_memory_space_constraint(a, pltpu.VMEM) for a in outcome[:3]),
        *(pltpu.with_memory_space_constraint(a, pltpu.SMEM) for a in outcome[3:]),
    )


def solution(mesh):
    return jax.shard_map(
        on_device,
        mesh=mesh,
        in_specs=(P(("grp", "dev"), None, None), P(), P(), P(), P(("grp", "dev"))),
        out_specs=P(("grp", "dev"), None, None),
        check_vma=False,
    )
```

```python
import functools
import itertools

import jax
import jax.numpy as jnp
from jax import lax
from jax.experimental import pallas as pl
from jax.experimental.pallas import tpu as pltpu
from jax.sharding import PartitionSpec as P

MESH = pl.DeviceIdType.MESH
SIDE = 4
CHIPS = SIDE**3
DEVICES = 2 * CHIPS
GROUP = 8
EDGE_GROUP = 1

STEPS = sorted(
    itertools.product(range(SIDE), repeat=3),
    key=lambda steps: (2 not in steps, -sum(min(step, SIDE - step) for step in steps)),
)
FAR = sum(2 in steps for steps in STEPS)
PACKED = [
    sum((STEPS[at + k][0] * 16 + STEPS[at + k][1] * 4 + STEPS[at + k][2]) << (6 * k) for k in range(4))
    for at in range(0, CHIPS, 4)
]
STAGES = [(0, (FAR, CHIPS), (0, 1)), (0, (0, FAR), (0, 1))] + [
    (group, (0, CHIPS), (turn,)) for group in (1, 2) for turn in range(2)
]


def how_many(stage):
    _, (low, high), turns = stage
    return sum(high - low - (turn == 0 and high == CHIPS) for turn in turns)


def visit_all(stage, me, visit):
    _, (low, high), turns = stage
    core, y, x, z = me

    def one(index, carry):
        number = PACKED[0]
        for k, packed in enumerate(PACKED[1:], 1):
            number = jnp.where(index >> 2 == k, packed, number)
        number = number >> (6 * (index & 3))
        chip = (((y + (number >> 4)) & 3) * SIDE + ((x + (number >> 2)) & 3)) * SIDE + ((z + number) & 3)
        for turn in turns:
            visit(((core + turn) & 1, chip))
        return carry

    if len(turns) == 1:
        lax.fori_loop(low, min(high, CHIPS - (turns[0] == 0)), one, 0)
        return
    lax.fori_loop(low, min(high, CHIPS - 1), one, 0)
    if high == CHIPS:
        visit(((core + 1) & 1, (y * SIDE + x) * SIDE + z))


def number_of(device):
    return device[0] * CHIPS + device[1]


def device_of(number):
    return number // CHIPS, number % CHIPS


def smooth(recv, out, first_field, left, tables, slots, carry=None):
    from_smem, take_smem, keep_smem = tables
    capacity, cells = out.shape[0], out.shape[2]
    at_lane = lax.broadcasted_iota(jnp.int32, (GROUP, cells), 1)
    first_lane, last_lane = at_lane == 0, at_lane == cells - 1

    def both(index):
        rank = int(index >= capacity // 2)
        block = recv[from_smem[index], rank * GROUP : (rank + 1) * GROUP] * take_smem[index]
        return block, pltpu.roll(block, 1, 1), pltpu.roll(block, cells - 1, 1)

    if carry is None:
        carry = both(0), left
    for index in slots:
        (current, to_right, to_left), previous = carry
        following = both(index + 1)
        cell_before = jnp.where(first_lane, previous, to_right)
        cell_after = jnp.where(last_lane, following[2], to_left)
        smoothed = ((current + current) + (cell_before + cell_after)) * keep_smem[index]
        out[index, first_field : first_field + GROUP] = smoothed
        carry = following, to_right
    return carry


def finish(parts, done, recv, left, from_smem, take_smem, keep_smem, out_hbm, last, done_sem, last_sem):
    capacity, ready, _ = done.shape
    rows = capacity // parts
    whole = [
        pltpu.make_async_copy(
            done.at[pl.ds(part * rows, rows)],
            out_hbm.at[pl.ds(part * rows, rows), pl.ds(0, ready)],
            done_sem.at[part],
        )
        for part in range(parts)
    ]
    for copy in whole:
        copy.start()
    carry, rest = None, []
    for part in range(parts):
        slots = range(part * rows, (part + 1) * rows)
        carry = smooth(recv, last, 0, left[...], (from_smem, take_smem, keep_smem), slots, carry)
        copy = pltpu.make_async_copy(
            last.at[pl.ds(part * rows, rows)],
            out_hbm.at[pl.ds(part * rows, rows), pl.ds(ready, GROUP)],
            last_sem.at[part],
        )
        copy.start()
        rest.append(copy)
    for copy in whole + rest:
        copy.wait()


def kernel(
    accum_hbm,
    slot_hbm,
    length_hbm,
    wet_hbm,
    count_hbm,
    out_ref,
    recv_2,
    left_ref,
    from_smem,
    take_smem,
    keep_smem,
    accum,
    slot,
    length_ref,
    send_0,
    send_1,
    send_2,
    recv_0,
    recv_1,
    edge_rows,
    wet_send,
    wet_recv,
    picks,
    picks_smem,
    slot_smem,
    wet_smem,
    count_smem,
    load_sem,
    picks_sem,
    send_sem,
    recv_sem,
    wet_send_sem,
    wet_recv_sem,
    ready_sem,
):
    sends, recvs = (send_0, send_1, send_2), (recv_0, recv_1, recv_2)
    groups = len(sends)
    blocks, fields, cells = accum.shape
    core, chip = lax.axis_index("grp"), lax.axis_index("dev")
    me = (core, chip // (SIDE * SIDE), (chip // SIDE) % SIDE, chip % SIDE)
    mine = core * CHIPS + chip

    loads = [
        pltpu.make_async_copy(src, dst, load_sem.at[number])
        for number, (src, dst) in enumerate(
            (
                (slot_hbm, slot),
                (length_hbm, length_ref),
                (accum_hbm, accum),
                (count_hbm, count_smem),
                (wet_hbm, wet_smem),
                (slot_hbm, slot_smem),
            )
        )
    ]
    for load in loads:
        load.start()
    barrier = pltpu.get_barrier_semaphore()

    def greet(other):
        pl.semaphore_signal(barrier, 1, device_id=other, device_id_type=MESH)

    visit_all(STAGES[0], me, greet)

    for load in loads[:2]:
        load.wait()
    row = lax.broadcasted_iota(jnp.int32, (128, 128), 0)
    lane = lax.broadcasted_iota(jnp.int32, (128, 128), 1)
    length = length_ref[...]
    length_col = jnp.sum(jnp.where(row == lane, length, 0), axis=1, keepdims=True)
    end = jnp.sum(jnp.where(row <= lane, length_col, 0), axis=0, keepdims=True)
    start = end - length
    slots = slot[...]
    held = (slots >> 7) == mine
    column = jnp.sum(jnp.where(held, lane, 0), axis=1, keepdims=True)
    local = jnp.sum(jnp.where(held, slots & 127, 0), axis=1, keepdims=True)
    order = row * 128 + column - start
    inside = (order >= 0) & (order < length)
    ahead, behind = order == -1, order == length
    for number, chosen in enumerate((inside & (order < 128), inside & (order >= 128), ahead, behind)):
        picks[number : number + 1, :] = jnp.sum(jnp.where(chosen, local, 0), axis=0, keepdims=True)
    picks_copy = pltpu.make_async_copy(picks, picks_smem, picks_sem)
    picks_copy.start()
    has_ahead = jnp.sum(jnp.where(ahead, 1.0, 0.0), axis=0, keepdims=True)
    has_behind = jnp.sum(jnp.where(behind, 1.0, 0.0), axis=0, keepdims=True)
    at_me = lax.broadcasted_iota(jnp.int32, (1, 128), 1) == mine
    my_start = jnp.sum(jnp.where(at_me, start, 0))
    my_length = jnp.sum(jnp.where(at_me, length, 0))
    final = jnp.maximum(my_length, 1) - 1

    for load in loads[3:5]:
        load.wait()
    at_field = lax.broadcasted_iota(jnp.int32, (GROUP, cells), 0)
    scales = []
    for group in range(groups):
        count = jnp.ones((GROUP, cells), jnp.int32)
        for field in range(GROUP):
            count = jnp.where(at_field == field, count_smem[group * GROUP + field], count)
        scales.append(0.25 / count.astype(jnp.float32))

    def is_wet(index):
        return wet_smem[index >> 7, index & 127] == 1

    wet_send[0] = jnp.full((GROUP, cells), jnp.where(is_wet(final), 1.0, 0.0), jnp.float32)
    wet_send[1] = jnp.full((GROUP, cells), jnp.where(is_wet(0), 1.0, 0.0), jnp.float32)

    picks_copy.wait()
    loads[2].wait()

    def pack(group):
        fields_of = slice(group * GROUP, (group + 1) * GROUP)

        def one(owner, carry):
            for rank in range(2):
                block = accum[picks_smem[rank, owner], fields_of]
                sends[group][owner, rank * GROUP : (rank + 1) * GROUP] = block * scales[group]
            return carry

        lax.fori_loop(0, DEVICES, one, 0, unroll=16)

    def keep_mine(group):
        recvs[group][mine] = sends[group][mine]

    def post(stage):
        group = STAGES[stage][0]

        def to(other):
            pltpu.make_async_remote_copy(
                src_ref=sends[group].at[number_of(other)],
                dst_ref=recvs[group].at[mine],
                send_sem=send_sem.at[stage],
                recv_sem=recv_sem.at[group],
                device_id=other,
                device_id_type=MESH,
            ).start()

        visit_all(STAGES[stage], me, to)

    def sent(stage):
        part = sends[STAGES[stage][0]].at[pl.ds(0, how_many(STAGES[stage]))]
        pltpu.make_async_copy(part, part, send_sem.at[stage]).wait()

    pack(0)
    keep_mine(0)
    pl.semaphore_wait(barrier, how_many(STAGES[0]))
    corners = [steps for steps in itertools.product(range(2), repeat=3) if any(steps)]
    for steps in corners:
        y, x, z = ((at + step) % SIDE for at, step in zip(me[1:], steps))
        pl.semaphore_signal(
            ready_sem, 1, device_id=(core, (y * SIDE + x) * SIDE + z), device_id_type=MESH
        )
    wet_copies = []
    for side, step in enumerate((1, DEVICES - 1)):
        copy = pltpu.make_async_remote_copy(
            src_ref=wet_send.at[side],
            dst_ref=wet_recv.at[side],
            send_sem=wet_send_sem.at[side],
            recv_sem=wet_recv_sem.at[side],
            device_id=device_of((mine + step) % DEVICES),
            device_id_type=MESH,
        )
        copy.start()
        wet_copies.append(copy)
    post(0)
    pl.semaphore_wait(ready_sem, len(corners))
    post(1)

    all_scales = jnp.concatenate(scales, axis=0)
    wide_lane = lax.broadcasted_iota(jnp.int32, (fields, cells), 1)

    def collect(owner, carry):
        cells_ahead, cells_behind = carry
        here = wide_lane == owner
        last = accum[picks_smem[2, owner]][:, cells - 1 : cells]
        first = accum[picks_smem[3, owner]][:, 0:1]
        return jnp.where(here, last, cells_ahead), jnp.where(here, first, cells_behind)

    nothing = jnp.zeros((fields, cells), jnp.float32)
    cells_ahead, cells_behind = lax.fori_loop(0, DEVICES, collect, (nothing, nothing), unroll=8)
    gathered = jnp.concatenate(
        [
            cells_ahead * all_scales * has_ahead,
            cells_behind * all_scales * has_behind,
            jnp.zeros((128 - 2 * fields, cells), jnp.float32),
        ],
        axis=0,
    )
    edge_rows[...] = gathered.T

    def attach(owner, carry):
        sends[EDGE_GROUP][owner, 2 * GROUP : 2 * GROUP + 1] = edge_rows[pl.ds(owner, 1)]
        return carry

    lax.fori_loop(0, DEVICES, attach, 0, unroll=16)
    for group in range(1, groups):
        pack(group)
        keep_mine(group)

    loads[5].wait()

    def table(index, carry):
        block = jnp.minimum(my_start + index, DEVICES * blocks - 1)
        behind_me = index == my_length
        from_smem[index] = jnp.where(behind_me, DEVICES, slot_smem[block >> 7, block & 127] >> 7)
        keep = jnp.where((index < my_length) & is_wet(index), 1.0, 0.0)
        keep_smem[index] = keep
        take_smem[index] = jnp.where(behind_me, 1.0, keep)
        return carry

    capacity = out_ref.shape[0]
    lax.fori_loop(0, capacity, table, 0, unroll=16)
    from_smem[capacity] = DEVICES
    take_smem[capacity] = 1.0

    at_lane = lax.broadcasted_iota(jnp.int32, (GROUP, cells), 1)
    first_lane, last_lane = at_lane == 0, at_lane == cells - 1

    def arrived(group):
        those = recvs[group].at[pl.ds(0, DEVICES - 1)]
        pltpu.make_async_copy(those, those, recv_sem.at[group]).wait()

    def edges():
        def add(sender, carry):
            return carry + recvs[EDGE_GROUP][sender, 2 * GROUP : 2 * GROUP + 1]

        total = lax.fori_loop(0, DEVICES, add, jnp.zeros((1, cells), jnp.float32), unroll=16)
        lefts = []
        for group in range(groups):
            left, right = (
                jnp.sum(jnp.where(at_lane == at_field + side * fields + group * GROUP, total, 0.0), axis=1, keepdims=True)
                for side in range(2)
            )
            lefts.append(left * wet_recv[0])
            for rank in range(2):
                recvs[group][DEVICES, rank * GROUP : (rank + 1) * GROUP] = right * wet_recv[1]
        return lefts

    for stage in range(2):
        sent(stage)
        post(stage + 2)
    arrived(0)
    for stage in range(2, 4):
        sent(stage)
        post(stage + 2)
    arrived(1)
    for copy in wet_copies:
        copy.wait()
    lefts = edges()
    for group in range(2):
        tables = from_smem, take_smem, keep_smem
        smooth(recvs[group], out_ref, group * GROUP, lefts[group], tables, range(capacity))
    left_ref[...] = jnp.broadcast_to(lefts[2], left_ref.shape)
    arrived(2)
    sent(4)
    sent(5)


def on_device(accum, step_count, stretch_slot, span_length, wet_mask):
    blocks, fields, cells = accum.shape
    capacity = wet_mask.shape[0]
    groups = fields // GROUP
    heights = [2 * GROUP + (group == EDGE_GROUP) for group in range(groups)]
    arguments = (
        accum,
        stretch_slot.reshape(-1, 128),
        span_length.reshape(1, -1),
        wet_mask.reshape(-1, 128),
        step_count,
    )
    outcome = pl.pallas_call(
        kernel,
        out_shape=(
            pltpu.VMEM((capacity, fields - GROUP, cells), jnp.float32),
            pltpu.VMEM((DEVICES + 1, heights[2], cells), jnp.float32),
            pltpu.VMEM((GROUP, cells), jnp.float32),
            pltpu.SMEM((capacity + 1,), jnp.int32),
            pltpu.SMEM((capacity + 1,), jnp.float32),
            pltpu.SMEM((capacity,), jnp.float32),
        ),
        in_specs=[pl.BlockSpec(memory_space=pltpu.HBM)] * len(arguments),
        out_specs=[pl.BlockSpec(memory_space=pltpu.VMEM)] * 3 + [pl.BlockSpec(memory_space=pltpu.SMEM)] * 3,
        scratch_shapes=[
            pltpu.VMEM((blocks, fields, cells), jnp.float32),
            pltpu.VMEM((128, 128), jnp.int32),
            pltpu.VMEM((1, 128), jnp.int32),
            *[pltpu.VMEM((DEVICES, height, cells), jnp.float32) for height in heights],
            *[pltpu.VMEM((DEVICES + 1, height, cells), jnp.float32) for height in heights[:2]],
            pltpu.VMEM((128, cells), jnp.float32),
            pltpu.VMEM((2, GROUP, cells), jnp.float32),
            pltpu.VMEM((2, GROUP, cells), jnp.float32),
            pltpu.VMEM((4, 128), jnp.int32),
            pltpu.SMEM((4, 128), jnp.int32),
            pltpu.SMEM((128, 128), jnp.int32),
            pltpu.SMEM((capacity // 128, 128), jnp.int32),
            pltpu.SMEM((fields,), jnp.int32),
            pltpu.SemaphoreType.DMA((6,)),
            pltpu.SemaphoreType.DMA,
            pltpu.SemaphoreType.DMA((2 * groups,)),
            pltpu.SemaphoreType.DMA((groups,)),
            pltpu.SemaphoreType.DMA((2,)),
            pltpu.SemaphoreType.DMA((2,)),
            pltpu.SemaphoreType.REGULAR,
        ],
        compiler_params=pltpu.CompilerParams(
            collective_id=0, has_side_effects=True, vmem_limit_bytes=32 * 1024 * 1024
        ),
        name="remap",
    )(*(pltpu.with_memory_space_constraint(a, pltpu.HBM) for a in arguments))

    parts = 16
    return pl.pallas_call(
        functools.partial(finish, parts),
        out_shape=pltpu.HBM((capacity, fields, cells), jnp.float32),
        in_specs=[pl.BlockSpec(memory_space=pltpu.VMEM)] * 3 + [pl.BlockSpec(memory_space=pltpu.SMEM)] * 3,
        out_specs=pl.BlockSpec(memory_space=pltpu.HBM),
        scratch_shapes=[
            pltpu.VMEM((capacity, GROUP, cells), jnp.float32),
            pltpu.SemaphoreType.DMA((parts,)),
            pltpu.SemaphoreType.DMA((parts,)),
        ],
        compiler_params=pltpu.CompilerParams(vmem_limit_bytes=16 * 1024 * 1024),
        name="finish",
    )(
        *(pltpu.with_memory_space_constraint(a, pltpu.VMEM) for a in outcome[:3]),
        *(pltpu.with_memory_space_constraint(a, pltpu.SMEM) for a in outcome[3:]),
    )


def solution(mesh):
    return jax.shard_map(
        on_device,
        mesh=mesh,
        in_specs=(P(("grp", "dev"), None, None), P(), P(), P(), P(("grp", "dev"))),
        out_specs=P(("grp", "dev"), None, None),
        check_vma=False,
    )
```
